512 devices in a mesh: grp: 2 (over x_lo), dom: 256 (over z, y, x_hi, core).
Axes of the slice: x: 4 (x_hi: 2, x_lo: 2; x = x_hi * 2 + x_lo), y: 8, z: 8, core: 2. Of those that a mesh axis runs over, the one named last changes fastest.
Arguments:
- surplus: float32 [48, 64, 65536], P('grp', None, 'dom'), may hold values from -40 to 40
- levels: int32 [48, 3], P('grp'), may hold values from 0 to 3
Outputs:
- updated: float32 [48, 64, 65536], P('grp', None, 'dom')
- coefficients: float32 [48], replicated
The draws below stay inside these ranges and needn't reach their ends.
All inputs are finite; a program needn't handle non-finite values.
Results may differ from the reference program's by a relative error of at most 0.0003.
Values sent between devices are 32-bit elements; how exact they have to be, the bound alone decides.
No kernel may reach another device: no remote copies, remote signals or barrier semaphores. Data moves between devices by JAX's collectives and lax.ppermute only.
A program may use at most 64 MiB of HBM per device.

```python
import math
import jax
import jax.numpy as jnp
from jax import lax

GRIDS = 48
SUBSP = 64
NC = 65536


def draw_surplus(key, part):
    keys = jax.random.split(jax.random.fold_in(key, 11), 4)
    index = jnp.arange(SUBSP, dtype=jnp.int32)
    level_sum = (index // 16 + index // 4 % 4 + index % 4).astype(jnp.float32)
    position = jnp.arange(NC, dtype=jnp.float32) / float(max(NC - 1, 1))
    common = jax.random.normal(keys[0], (SUBSP, NC), jnp.float32)
    single = jax.random.normal(keys[1], (GRIDS, SUBSP, NC), jnp.float32)
    gains = jnp.exp(jax.random.uniform(keys[2], (GRIDS, SUBSP, 1), jnp.float32, math.log(0.5), math.log(2.0)))
    spread = jnp.exp(jax.random.uniform(keys[3], (GRIDS, SUBSP, 1), jnp.float32, math.log(0.4), math.log(1.2)))
    envelope = 3.0 ** position / math.sqrt(3.0)
    amplitude = 1.5 * 10.0 ** (-level_sum / 9.0)
    values = envelope[None, None, :] * amplitude[None, :, None] * (gains * common[None] + spread * single)
    return jnp.clip(values, -40.0, 40.0).astype(jnp.float32)


def set_ends(result, own_key, smallest, high):
    dims = result.shape
    index_at = [jax.random.randint(jax.random.fold_in(own_key, axis), (), 0, dims[axis]) for axis in range(len(dims))]
    result = result.at[tuple(index_at)].set(smallest)
    longest = dims.index(max(dims))
    index_at[longest] = (index_at[longest] + 1) % dims[longest]
    return result.at[tuple(index_at)].set(high)


def setup_inputs(seed: int = 0) -> dict:
    arg_keys = jax.random.split(jax.random.key(seed), 3)
    return {
        "surplus": draw_surplus(jax.random.fold_in(arg_keys[2], 71), 0),
        "levels": set_ends(jax.random.randint(arg_keys[1], (GRIDS, 3), 0, 4), jax.random.fold_in(arg_keys[1], 1), 0, 3).astype(jnp.int32),
    }


def owned(levels, count):
    indices = jnp.arange(count, dtype=jnp.int32)
    digits = jnp.stack([indices // 16, indices // 4 % 4, indices % 4])
    return jnp.all(digits[None] <= levels[:, :, None], axis=1).astype(jnp.float32)

def solve_weights(gram_matrix):
    number = gram_matrix.shape[0]
    diagonal_part = jnp.diagonal(gram_matrix) + 1e-06
    scaling = 1.0 / jnp.sqrt(diagonal_part)
    system = scaling[:, None] * gram_matrix * scaling[None, :] + 0.1 * jnp.eye(number, dtype=jnp.float32)
    factor = jnp.linalg.cholesky(system)
    target = jnp.sqrt(diagonal_part)[:, None]
    halfway = lax.linalg.triangular_solve(factor, target, left_side=True, lower=True)
    weights = lax.linalg.triangular_solve(factor, halfway, left_side=True, lower=True, transpose_a=True)
    return scaling * weights[:, 0]

def reference(surplus, levels):
    owners = owned(levels, SUBSP)
    masked = surplus * owners[:, :, None]
    flattened = masked.reshape(GRIDS, -1)
    gram_matrix = jnp.dot(flattened.astype(jnp.float32), flattened.T.astype(jnp.float32), precision=lax.Precision.HIGHEST, preferred_element_type=jnp.float32)
    coefficients = solve_weights(gram_matrix)
    combined = jnp.tensordot(coefficients, masked, axes=1, precision=lax.Precision.HIGHEST)
    updated = owners[:, :, None] * combined[None]
    return (updated, coefficients)
```

```python
import jax
import jax.numpy as jnp
from jax import lax
from jax.sharding import Mesh
from jax.sharding import PartitionSpec as P

DOM = ("dom_0", "dom_1", "dom_2", "dom_3")
STAGES = (("dom_0",), ("dom_1",), ("grp", "dom_2", "dom_3"))
SWAP = ((0, 1), (1, 0))


def owned(levels, count):
    indices = jnp.arange(count, dtype=jnp.int32)
    digits = jnp.stack([indices // 16, indices // 4 % 4, indices % 4])
    return jnp.all(digits[None] <= levels[:, :, None], axis=1).astype(jnp.float32)


def solve_weights(gram_matrix):
    number = gram_matrix.shape[0]
    diagonal_part = jnp.diagonal(gram_matrix) + 1e-06
    scaling = 1.0 / jnp.sqrt(diagonal_part)
    system = scaling[:, None] * gram_matrix * scaling[None, :] + 0.1 * jnp.eye(
        number, dtype=jnp.float32
    )
    factor = jnp.linalg.cholesky(system)
    target = jnp.sqrt(diagonal_part)[:, None]
    halfway = lax.linalg.triangular_solve(factor, target, left_side=True, lower=True)
    weights = lax.linalg.triangular_solve(
        factor, halfway, left_side=True, lower=True, transpose_a=True
    )
    return scaling * weights[:, 0]


def inner(left, right):
    return lax.dot_general(
        left,
        right,
        (((1, 2), (1, 2)), ((), ())),
        precision=lax.Precision.HIGHEST,
        preferred_element_type=jnp.float32,
    )


def summed(array, axes):
    count = lax.axis_size(axes)
    copies = jnp.broadcast_to(array, (count, *array.shape))
    return jnp.sum(lax.all_to_all(copies, axes, split_axis=0, concat_axis=0, tiled=True), axis=0)


def weighted(weights, grids):
    return jnp.sum(weights[:, None, None] * grids, axis=0)


def shards(surplus, levels):
    local, subspaces, cells = surplus.shape
    half = cells // 2
    second = lax.axis_index("grp") == 1
    owners = owned(levels, subspaces)
    masked = surplus * owners[:, :, None]
    low, high = masked[:, :, :half], masked[:, :, half:]
    near = jnp.where(second, high, low)
    far = jnp.where(second, low, high)
    got_near = lax.ppermute(far, "grp", SWAP)
    got_far = lax.ppermute(near, "grp", SWAP)
    own_block = inner(masked, masked)
    cross = inner(near, got_near)
    cross = jnp.where(second, cross.T, cross)
    zero = jnp.zeros_like(own_block)
    parts = jnp.concatenate(
        [
            jnp.where(second, zero, own_block),
            cross,
            jnp.where(second, own_block, zero),
            jnp.zeros((local, 128 - 3 * local), jnp.float32),
        ],
        axis=1,
    )
    for axes in STAGES:
        parts = summed(parts, axes)
    first, cross, last = (parts[:, k * local : (k + 1) * local] for k in range(3))
    gram_matrix = jnp.concatenate(
        [jnp.concatenate([first, cross], axis=1), jnp.concatenate([cross.T, last], axis=1)], axis=0
    )
    coefficients = solve_weights(gram_matrix)
    start, stop = coefficients[:local], coefficients[local:]
    own = jnp.where(second, stop, start)
    other = jnp.where(second, start, stop)
    sum_near = weighted(own, near) + weighted(other, got_near)
    sum_far = weighted(own, far) + weighted(other, got_far)
    combined = jnp.concatenate(
        [jnp.where(second, sum_far, sum_near), jnp.where(second, sum_near, sum_far)], axis=1
    )
    return owners[:, :, None] * combined[None], coefficients


def solution(mesh):
    torus = Mesh(
        mesh.devices.reshape(mesh.shape["grp"], 8, 8, 2, 2),
        ("grp", *DOM),
    )
    return jax.shard_map(
        shards,
        mesh=torus,
        in_specs=(P("grp", None, DOM), P("grp", None)),
        out_specs=(P("grp", None, DOM), P()),
        check_vma=False,
    )
```

```python
import jax
import jax.numpy as jnp
from jax import lax
from jax.experimental import pallas as pl
from jax.experimental.pallas import tpu as pltpu
from jax.sharding import Mesh
from jax.sharding import PartitionSpec as P

DOM = ("dom_0", "dom_1", "dom_2", "dom_3")
STAGES = (("dom_0",), ("dom_1",), ("grp", "dom_2", "dom_3"))
SWAP = ((0, 1), (1, 0))
LANES = 128


def owned(levels, count):
    indices = jnp.arange(count, dtype=jnp.int32)
    digits = jnp.stack([indices // 16, indices // 4 % 4, indices % 4])
    return jnp.all(digits[None] <= levels[:, :, None], axis=1).astype(jnp.float32)


def solve_kernel(parts_ref, out_ref):
    number = 2 * parts_ref.shape[1]
    folded = parts_ref[0]
    for k in range(1, parts_ref.shape[0]):
        folded = folded + parts_ref[k]
    gram = jnp.concatenate([folded, pltpu.roll(folded, LANES - number, 1)], axis=0)
    rows = lax.broadcasted_iota(jnp.int32, gram.shape, 0)
    lanes = lax.broadcasted_iota(jnp.int32, gram.shape, 1)
    on_diagonal = rows == lanes
    diagonal = jnp.sum(jnp.where(on_diagonal, gram, 0.0), axis=1, keepdims=True) + 1e-06
    system = jnp.where(lanes < number, gram, 0.0) + jnp.where(on_diagonal, 0.1 * diagonal, 0.0)
    system = jnp.where(lanes == number, diagonal, system)
    for k in range(number):
        row = system[k : k + 1, :]
        column = jnp.broadcast_to(system[:, k : k + 1], system.shape)
        scaled = row * (1.0 / column[k : k + 1, :])
        system = system - jnp.where(rows == k, 0.0, column) * jnp.broadcast_to(scaled, system.shape)
    last = jnp.broadcast_to(system[:, number : number + 1], system.shape)
    out_ref[...] = jnp.sum(jnp.where(on_diagonal, last / system, 0.0), axis=0, keepdims=True)


def solve_parts(parts):
    whole = pl.BlockSpec(memory_space=pltpu.VMEM)
    return pl.pallas_call(
        solve_kernel,
        out_shape=jax.ShapeDtypeStruct((1, LANES), jnp.float32),
        in_specs=[whole],
        out_specs=whole,
    )(parts)


def inner(left, right):
    return lax.dot_general(
        left,
        right,
        (((1, 2), (1, 2)), ((), ())),
        precision=lax.Precision.HIGHEST,
        preferred_element_type=jnp.float32,
    )


def exchanged(array, axes):
    copies = jnp.broadcast_to(array, (lax.axis_size(axes), *array.shape))
    return lax.all_to_all(copies, axes, split_axis=0, concat_axis=0, tiled=True)


def weighted(weights, grids):
    return jnp.sum(weights[:, None, None] * grids, axis=0)


def shards(surplus, levels):
    local, subspaces, cells = surplus.shape
    half = cells // 2
    second = lax.axis_index("grp") == 1
    owners = owned(levels, subspaces)
    masked = surplus * owners[:, :, None]
    low, high = masked[:, :, :half], masked[:, :, half:]
    near = jnp.where(second, high, low)
    far = jnp.where(second, low, high)
    got_near = lax.ppermute(far, "grp", SWAP)
    got_far = lax.ppermute(near, "grp", SWAP)
    own_block = inner(masked, masked)
    cross = inner(near, got_near)
    zero = jnp.zeros_like(own_block)
    parts = jnp.concatenate(
        [
            jnp.where(second, zero, own_block),
            jnp.where(second, cross.T, cross),
            jnp.where(second, cross, cross.T),
            jnp.where(second, own_block, zero),
            jnp.zeros((local, LANES - 4 * local), jnp.float32),
        ],
        axis=1,
    )
    for axes in STAGES[:-1]:
        parts = jnp.sum(exchanged(parts, axes), axis=0)
    coefficients = solve_parts(exchanged(parts, STAGES[-1]))[0, : 2 * local]
    start, stop = coefficients[:local], coefficients[local:]
    own = jnp.where(second, stop, start)
    other = jnp.where(second, start, stop)
    sum_near = weighted(own, near) + weighted(other, got_near)
    sum_far = weighted(own, far) + weighted(other, got_far)
    combined = jnp.concatenate(
        [jnp.where(second, sum_far, sum_near), jnp.where(second, sum_near, sum_far)], axis=1
    )
    return owners[:, :, None] * combined[None], coefficients


def solution(mesh):
    torus = Mesh(
        mesh.devices.reshape(mesh.shape["grp"], 8, 8, 2, 2),
        ("grp", *DOM),
    )
    return jax.shard_map(
        shards,
        mesh=torus,
        in_specs=(P("grp", None, DOM), P("grp", None)),
        out_specs=(P("grp", None, DOM), P()),
        check_vma=False,
    )
```

```python
import jax
import jax.numpy as jnp
from jax import lax
from jax.experimental import pallas as pl
from jax.experimental.pallas import tpu as pltpu
from jax.sharding import Mesh
from jax.sharding import PartitionSpec as P

DOM = ("dom_0", "dom_1", "dom_2", "dom_3")
STAGES = (("dom_0",), ("dom_1",), ("grp", "dom_2", "dom_3"))
SWAP = ((0, 1), (1, 0))
LANES = 128
SUBSPACES = 64
TILES = 8
HEAD = 8
ROOM = 592
ROWS = HEAD + ROOM + 8
VMEM = pl.BlockSpec(memory_space=pltpu.VMEM)
SMEM = pl.BlockSpec(memory_space=pltpu.SMEM)
ANY = pl.BlockSpec(memory_space=pl.ANY)


def positions(levels, i, start):
    l0, l1, l2 = (levels[d, i].astype(jnp.int32) for d in range(3))
    width = l2 + 1
    rows = []
    for a in range(4):
        for b in range(4):
            at = jnp.minimum(start + (a * (l1 + 1) + b) * width, HEAD + ROOM)
            rows.append(jnp.where((a <= l0) & (b <= l1), at, HEAD + ROOM))
    return rows, start + (l0 + 1) * (l1 + 1) * width


def owner_tiles(levels, i):
    l0, l1, l2 = (levels[d, i].astype(jnp.int32) for d in range(3))
    row = lax.broadcasted_iota(jnp.int32, (8, LANES), 0)
    fits = (row & 3) <= l2
    return [fits & (k % 2 * 2 + (row >> 2) <= l1) & (k // 2 <= l0) for k in range(TILES)]


def tile_rows(i, k):
    return pl.ds(pl.multiple_of(i * SUBSPACES + k * 8, 8), 8)


def packed_tile(packed_ref, rows, k):
    row = lax.broadcasted_iota(jnp.int32, (8, LANES), 0)
    upper = packed_ref[pl.ds(rows[2 * k], 8), :]
    lower = packed_ref[pl.ds(rows[2 * k + 1] - 4, 8), :]
    return jnp.where(row < 4, upper, lower)


def half_copies(surplus_ref, held, sems):
    side = lax.axis_index("grp")

    def copy(i, slot):
        lanes = pl.ds(pl.multiple_of((1 - side if slot else side) * LANES, LANES), LANES)
        rows = pl.ds(i * SUBSPACES, SUBSPACES)
        return pltpu.make_async_copy(surplus_ref.at[i, :, lanes], held.at[slot, rows, :], sems.at[slot, i])

    return copy


def held_scratch(grids):
    return [
        pltpu.VMEM((2, grids * SUBSPACES, LANES), jnp.float32),
        pltpu.SemaphoreType.DMA((2, grids)),
    ]


def pack_kernel(levels_ref, surplus_ref, far_ref, near_ref, held, sems):
    grids = surplus_ref.shape[0]
    copy = half_copies(surplus_ref, held, sems)
    for i in range(grids):
        copy(i, 0).start()
        copy(i, 1).start()
    head = jnp.zeros((HEAD, LANES), jnp.float32)
    row = lax.broadcasted_iota(jnp.int32, head.shape, 0)
    lane = lax.broadcasted_iota(jnp.int32, head.shape, 1)
    for d in range(3):
        for i in range(grids):
            head = jnp.where((row == d) & (lane == i), levels_ref[d, i].astype(jnp.float32), head)
    far_ref[0:HEAD, :] = head
    near_ref[0:HEAD, :] = head

    def pack(i, start):
        copy(i, 0).wait()
        copy(i, 1).wait()
        rows, stop = positions(levels_ref, i, start)
        for k in range(TILES):
            for slot, out in ((0, near_ref), (1, far_ref)):
                tile = held[slot, tile_rows(i, k), :]
                out[pl.ds(rows[2 * k], 4), :] = tile[0:4]
                out[pl.ds(rows[2 * k + 1], 4), :] = tile[4:8]
        return stop

    lax.fori_loop(0, grids, pack, jnp.int32(HEAD))


def pack(levels, surplus):
    packed = jax.ShapeDtypeStruct((ROWS, LANES), jnp.float32)
    return pl.pallas_call(
        pack_kernel,
        out_shape=(packed, packed),
        in_specs=[SMEM, ANY],
        out_specs=(VMEM, VMEM),
        scratch_shapes=held_scratch(surplus.shape[0]),
    )(levels, surplus)


def products(left_ref, right_ref, grids):
    def pair(ref, s):
        rows = [ref[pl.ds(s + k, grids, stride=SUBSPACES), :] for k in range(2)]
        return jnp.concatenate(rows, axis=1)

    total = jnp.zeros((grids, grids), jnp.float32)
    for s in range(0, SUBSPACES, 2):
        total = total + lax.dot_general(
            pair(left_ref, s),
            pair(right_ref, s),
            (((1,), (1,)), ((), ())),
            precision=lax.Precision.HIGHEST,
            preferred_element_type=jnp.float32,
        )
    return total


def own_kernel(levels_ref, surplus_ref, near_ref, block_ref, held, sems, far_ref):
    grids = surplus_ref.shape[0]
    copy = half_copies(surplus_ref, held, sems)
    for i in range(grids):
        copy(i, 0).start()
        copy(i, 1).start()

    def mask(i, carry):
        copy(i, 0).wait()
        copy(i, 1).wait()
        tiles = owner_tiles(levels_ref, i)
        for k in range(TILES):
            at = tile_rows(i, k)
            near_ref[at, :] = jnp.where(tiles[k], held[0, at, :], 0.0)
            far_ref[at, :] = jnp.where(tiles[k], held[1, at, :], 0.0)
        return carry

    lax.fori_loop(0, grids, mask, 0)
    block_ref[...] = products(near_ref, near_ref, grids) + products(far_ref, far_ref, grids)


def own_products(levels, surplus):
    grids = surplus.shape[0]
    half = (grids * SUBSPACES, LANES)
    return pl.pallas_call(
        own_kernel,
        out_shape=(
            jax.ShapeDtypeStruct(half, jnp.float32),
            jax.ShapeDtypeStruct((grids, grids), jnp.float32),
        ),
        in_specs=[SMEM, ANY],
        out_specs=(VMEM, VMEM),
        scratch_shapes=[*held_scratch(grids), pltpu.VMEM(half, jnp.float32)],
    )(levels, surplus)


def fold(block, cross, turned, second):
    zero = jnp.zeros_like(block)
    return jnp.concatenate(
        [
            jnp.where(second, zero, block),
            jnp.where(second, turned, cross),
            jnp.where(second, cross, turned),
            jnp.where(second, block, zero),
            jnp.zeros((block.shape[0], LANES - 4 * block.shape[0]), jnp.float32),
        ],
        axis=1,
    )


def cross_kernel(levels_ref, near_ref, block_ref, got_ref, parts_ref, full_ref, other_ref, head, sem):
    grids = block_ref.shape[0]
    fetch = pltpu.make_async_copy(got_ref.at[0:HEAD, :], head, sem)
    fetch.start()
    own = jnp.int32(HEAD)
    for i in range(grids):
        own = own + (levels_ref[0, i] + 1) * (levels_ref[1, i] + 1) * (levels_ref[2, i] + 1)
    fetch.wait()

    def unpack(i, start):
        rows, stop = positions(head, i, start)
        tiles = owner_tiles(head, i)
        for k in range(TILES):
            tile = packed_tile(got_ref, rows, k)
            other_ref[tile_rows(i, k), :] = jnp.where(tiles[k], tile, 0.0)
        return stop

    stop = lax.fori_loop(0, grids, unpack, jnp.int32(HEAD))
    full_ref[0] = (jnp.maximum(own, stop) > HEAD + ROOM).astype(jnp.int32)
    cross = products(near_ref, other_ref, grids)
    folded = fold(block_ref[...], cross, cross.T, lax.axis_index("grp") == 1)
    for k in range(parts_ref.shape[0]):
        parts_ref[k] = folded


def cross_products(levels, near, block, got, copies):
    grids = block.shape[0]
    return pl.pallas_call(
        cross_kernel,
        out_shape=(
            jax.ShapeDtypeStruct((copies, grids, LANES), jnp.float32),
            jax.ShapeDtypeStruct((1,), jnp.int32),
        ),
        in_specs=[SMEM, VMEM, VMEM, VMEM],
        out_specs=(VMEM, SMEM),
        scratch_shapes=[
            pltpu.VMEM((grids * SUBSPACES, LANES), jnp.float32),
            pltpu.SMEM((HEAD, LANES), jnp.float32),
            pltpu.SemaphoreType.DMA,
        ],
    )(levels, near, block, got)


def eliminate(parts_ref):
    number = 2 * parts_ref.shape[1]
    folded = parts_ref[0]
    for k in range(1, parts_ref.shape[0]):
        folded = folded + parts_ref[k]
    gram = jnp.concatenate([folded, pltpu.roll(folded, LANES - number, 1)], axis=0)
    rows = lax.broadcasted_iota(jnp.int32, gram.shape, 0)
    lanes = lax.broadcasted_iota(jnp.int32, gram.shape, 1)
    on_diagonal = rows == lanes
    diagonal = jnp.sum(jnp.where(on_diagonal, gram, 0.0), axis=1, keepdims=True) + 1e-06
    system = jnp.where(lanes < number, gram, 0.0) + jnp.where(on_diagonal, 0.1 * diagonal, 0.0)
    system = jnp.where(lanes == number, diagonal, system)
    for k in range(number):
        row = system[k : k + 1, :]
        column = jnp.broadcast_to(system[:, k : k + 1], system.shape)
        scaled = row * (1.0 / column[k : k + 1, :])
        system = system - jnp.where(rows == k, 0.0, column) * jnp.broadcast_to(scaled, system.shape)
    last = jnp.broadcast_to(system[:, number : number + 1], system.shape)
    solved = jnp.where(on_diagonal, last / system, 0.0)
    return jnp.broadcast_to(jnp.sum(solved, axis=1, keepdims=True), system.shape), on_diagonal


def solve_kernel(parts_ref, out_ref):
    solution_rows, on_diagonal = eliminate(parts_ref)
    out_ref[...] = jnp.sum(jnp.where(on_diagonal, solution_rows, 0.0), axis=0, keepdims=True)


def solve_parts(parts):
    return pl.pallas_call(
        solve_kernel,
        out_shape=jax.ShapeDtypeStruct((1, LANES), jnp.float32),
        in_specs=[VMEM],
        out_specs=VMEM,
    )(parts)


def finish_kernel(
    levels_ref,
    parts_ref,
    surplus_ref,
    got_near_ref,
    got_far_ref,
    updated_ref,
    out_ref,
    held,
    sems,
    head,
    head_sem,
    weights,
    result,
    out_sems,
):
    grids = surplus_ref.shape[0]
    side = lax.axis_index("grp")
    copy = half_copies(surplus_ref, held, sems)
    fetch = pltpu.make_async_copy(got_near_ref.at[0:HEAD, :], head, head_sem)
    fetch.start()
    for i in range(grids):
        copy(i, 0).start()
        copy(i, 1).start()
    solution_rows, on_diagonal = eliminate(parts_ref)
    out_ref[...] = jnp.sum(jnp.where(on_diagonal, solution_rows, 0.0), axis=0, keepdims=True)
    weights[...] = solution_rows
    fetch.wait()

    def add(i, carry):
        start, sums = carry
        copy(i, 0).wait()
        copy(i, 1).wait()
        rows, stop = positions(head, i, start)
        own_tiles = owner_tiles(levels_ref, i)
        other_tiles = owner_tiles(head, i)
        own = jnp.broadcast_to(weights[pl.ds(side * grids + i, 1), :], (8, LANES))
        other = jnp.broadcast_to(weights[pl.ds((1 - side) * grids + i, 1), :], (8, LANES))
        added = []
        for slot, got in ((0, got_near_ref), (1, got_far_ref)):
            for k in range(TILES):
                mine = jnp.where(own_tiles[k], held[slot, tile_rows(i, k), :], 0.0)
                theirs = jnp.where(other_tiles[k], packed_tile(got, rows, k), 0.0)
                added.append(sums[slot * TILES + k] + own * mine + other * theirs)
        return stop, tuple(added)

    zero = jnp.zeros((8, LANES), jnp.float32)
    _, sums = lax.fori_loop(0, grids, add, (jnp.int32(HEAD), (zero,) * (2 * TILES)))

    def put(i, slot):
        lanes = pl.ds(pl.multiple_of((1 - side if slot else side) * LANES, LANES), LANES)
        rows = pl.ds(i * SUBSPACES, SUBSPACES)
        return pltpu.make_async_copy(result.at[slot, rows, :], updated_ref.at[i, :, lanes], out_sems.at[slot, i])

    def spread(i, carry):
        tiles = owner_tiles(levels_ref, i)
        for slot in range(2):
            for k in range(TILES):
                result[slot, tile_rows(i, k), :] = jnp.where(tiles[k], sums[slot * TILES + k], 0.0)
            put(i, slot).start()
        return carry

    lax.fori_loop(0, grids, spread, 0)
    for i in range(grids):
        put(i, 0).wait()
        put(i, 1).wait()


def finish(levels, parts, surplus, got_near, got_far):
    grids = surplus.shape[0]
    return pl.pallas_call(
        finish_kernel,
        out_shape=(
            jax.ShapeDtypeStruct(surplus.shape, jnp.float32),
            jax.ShapeDtypeStruct((1, LANES), jnp.float32),
        ),
        in_specs=[SMEM, VMEM, ANY, VMEM, VMEM],
        out_specs=(ANY, VMEM),
        scratch_shapes=[
            *held_scratch(grids),
            pltpu.SMEM((HEAD, LANES), jnp.float32),
            pltpu.SemaphoreType.DMA,
            pltpu.VMEM((2 * grids, LANES), jnp.float32),
            *held_scratch(grids),
        ],
    )(levels, parts, surplus, got_near, got_far)


def owned(levels, count):
    indices = jnp.arange(count, dtype=jnp.int32)
    digits = jnp.stack([indices // 16, indices // 4 % 4, indices % 4])
    return jnp.all(digits[:, None] <= levels[:, :, None], axis=0).astype(jnp.float32)


def halves(levels, surplus):
    second = lax.axis_index("grp") == 1
    masked = surplus * owned(levels, SUBSPACES)[:, :, None]
    low, high = masked[:, :, :LANES], masked[:, :, LANES:]
    return jnp.where(second, high, low), jnp.where(second, low, high)


def dense_parts(levels, surplus, block, copies):
    near, far = halves(levels, surplus)
    cross = lax.dot_general(
        near,
        lax.ppermute(far, "grp", SWAP),
        (((1, 2), (1, 2)), ((), ())),
        precision=lax.Precision.HIGHEST,
        preferred_element_type=jnp.float32,
    )
    folded = fold(block, cross, cross.T, lax.axis_index("grp") == 1)
    return jnp.broadcast_to(folded, (copies, *folded.shape))


def dense_finish(levels, parts, surplus):
    grids = surplus.shape[0]
    second = lax.axis_index("grp") == 1
    near, far = halves(levels, surplus)
    got_near = lax.ppermute(far, "grp", SWAP)
    got_far = lax.ppermute(near, "grp", SWAP)
    coefficients = solve_parts(parts)
    start, stop = coefficients[0, :grids], coefficients[0, grids : 2 * grids]
    own = jnp.where(second, stop, start)[:, None, None]
    other = jnp.where(second, start, stop)[:, None, None]
    sum_near = jnp.sum(own * near + other * got_near, axis=0)
    sum_far = jnp.sum(own * far + other * got_far, axis=0)
    combined = jnp.concatenate(
        [jnp.where(second, sum_far, sum_near), jnp.where(second, sum_near, sum_far)], axis=1
    )
    return owned(levels, SUBSPACES)[:, :, None] * combined[None], coefficients


def exchanged(copies, axes):
    return lax.all_to_all(copies, axes, split_axis=0, concat_axis=0, tiled=True)


def shards(surplus, levels):
    grids = surplus.shape[0]
    levels = levels.T
    far, near = pack(levels, surplus)
    got_near = lax.ppermute(far, "grp", SWAP)
    got_far = lax.ppermute(near, "grp", SWAP)
    own, block = own_products(levels, surplus)
    parts, full = cross_products(levels, own, block, got_near, lax.axis_size(STAGES[0]))
    dense = full[0] > 0
    parts = lax.cond(
        dense, lambda: dense_parts(levels, surplus, block, parts.shape[0]), lambda: parts
    )
    for axes, following in zip(STAGES, STAGES[1:]):
        folded = jnp.sum(exchanged(parts, axes), axis=0)
        parts = jnp.broadcast_to(folded, (lax.axis_size(following), *folded.shape))
    parts = exchanged(parts, STAGES[-1])
    updated, coefficients = lax.cond(
        dense,
        lambda: dense_finish(levels, parts, surplus),
        lambda: tuple(finish(levels, parts, surplus, got_near, got_far)),
    )
    return updated, coefficients[0, : 2 * grids]


def solution(mesh):
    torus = Mesh(
        mesh.devices.reshape(mesh.shape["grp"], 8, 8, 2, 2),
        ("grp", *DOM),
    )
    return jax.shard_map(
        shards,
        mesh=torus,
        in_specs=(P("grp", None, DOM), P("grp", None)),
        out_specs=(P("grp", None, DOM), P()),
        check_vma=False,
    )
```

```python
import jax
import jax.numpy as jnp
from jax import lax
from jax.experimental import pallas as pl
from jax.experimental.pallas import tpu as pltpu
from jax.sharding import Mesh
from jax.sharding import PartitionSpec as P

DOM = ("z_hi", "z_lo", "y_hi", "y_lo", "x_hi", "core")
STAGES = (("z_hi", "y_hi"), ("grp", "x_hi", "core", "z_lo", "y_lo"))
SWAP = ((0, 1), (1, 0))
LANES = 128
SUBSPACES = 64
TILES = 8
HEAD = 8
ROOM = 592
ROWS = HEAD + ROOM + 8
VMEM = pl.BlockSpec(memory_space=pltpu.VMEM)
SMEM = pl.BlockSpec(memory_space=pltpu.SMEM)
ANY = pl.BlockSpec(memory_space=pl.ANY)


def positions(levels, i, start):
    l0, l1, l2 = (levels[d, i].astype(jnp.int32) for d in range(3))
    width = l2 + 1
    rows = []
    for a in range(4):
        for b in range(4):
            at = jnp.minimum(start + (a * (l1 + 1) + b) * width, HEAD + ROOM)
            rows.append(jnp.where((a <= l0) & (b <= l1), at, HEAD + ROOM))
    return rows, start + (l0 + 1) * (l1 + 1) * width


def owner_tiles(levels, i):
    l0, l1, l2 = (levels[d, i].astype(jnp.int32) for d in range(3))
    row = lax.broadcasted_iota(jnp.int32, (8, LANES), 0)
    fits = (row & 3) <= l2
    return [fits & (k % 2 * 2 + (row >> 2) <= l1) & (k // 2 <= l0) for k in range(TILES)]


def tile_rows(i, k):
    return pl.ds(pl.multiple_of(i * SUBSPACES + k * 8, 8), 8)


def packed_tile(packed_ref, rows, k):
    row = lax.broadcasted_iota(jnp.int32, (8, LANES), 0)
    upper = packed_ref[pl.ds(rows[2 * k], 8), :]
    lower = packed_ref[pl.ds(rows[2 * k + 1] - 4, 8), :]
    return jnp.where(row < 4, upper, lower)


def half_lanes(slot):
    side = lax.axis_index("grp")
    return pl.ds(pl.multiple_of((1 - side if slot else side) * LANES, LANES), LANES)


def cell_tile(surplus_ref, i, k, slot):
    return surplus_ref[i, k * 8 : k * 8 + 8, half_lanes(slot)]


def store_packed(out_ref, rows, k, tile):
    out_ref[pl.ds(rows[2 * k], 4), :] = tile[0:4]
    out_ref[pl.ds(rows[2 * k + 1], 4), :] = tile[4:8]


def pack_far_kernel(levels_ref, surplus_ref, out_ref, held, sems):
    grids = surplus_ref.shape[0]

    def copy(i):
        rows = pl.ds(i * SUBSPACES, SUBSPACES)
        return pltpu.make_async_copy(surplus_ref.at[i, :, half_lanes(1)], held.at[rows, :], sems.at[i])

    for i in range(grids):
        copy(i).start()
    head = jnp.zeros((HEAD, LANES), jnp.float32)
    row = lax.broadcasted_iota(jnp.int32, head.shape, 0)
    lane = lax.broadcasted_iota(jnp.int32, head.shape, 1)
    for d in range(3):
        for i in range(grids):
            head = jnp.where((row == d) & (lane == i), levels_ref[d, i].astype(jnp.float32), head)
    out_ref[0:HEAD, :] = head

    def pack(i, start):
        copy(i).wait()
        rows, stop = positions(levels_ref, i, start)
        for k in range(TILES):
            store_packed(out_ref, rows, k, held[tile_rows(i, k), :])
        return stop

    lax.fori_loop(0, grids, pack, jnp.int32(HEAD))


def pack_far(levels, surplus):
    grids = surplus.shape[0]
    return pl.pallas_call(
        pack_far_kernel,
        out_shape=jax.ShapeDtypeStruct((ROWS, LANES), jnp.float32),
        in_specs=[SMEM, ANY],
        out_specs=VMEM,
        scratch_shapes=[
            pltpu.VMEM((grids * SUBSPACES, LANES), jnp.float32),
            pltpu.SemaphoreType.DMA((grids,)),
        ],
    )(levels, surplus)


def pack_near_kernel(levels_ref, surplus_ref, out_ref):
    grids = surplus_ref.shape[0]
    out_ref[0:HEAD, :] = jnp.zeros((HEAD, LANES), jnp.float32)

    def pack(i, start):
        rows, stop = positions(levels_ref, i, start)
        for k in range(TILES):
            store_packed(out_ref, rows, k, cell_tile(surplus_ref, i, k, 0))
        return stop

    lax.fori_loop(0, grids, pack, jnp.int32(HEAD))


def pack_near(levels, surplus):
    return pl.pallas_call(
        pack_near_kernel,
        out_shape=jax.ShapeDtypeStruct((ROWS, LANES), jnp.float32),
        in_specs=[SMEM, VMEM],
        out_specs=VMEM,
    )(levels, surplus)


def products(left_ref, right_ref, grids):
    def split(ref, s):
        rows = [ref[pl.ds(s + k, grids, stride=SUBSPACES), :] for k in range(8)]
        rows = jnp.concatenate(rows, axis=1)
        high = rows.astype(jnp.bfloat16)
        return high, (rows - high.astype(jnp.float32)).astype(jnp.bfloat16)

    total = jnp.zeros((grids, grids), jnp.float32)
    for s in range(0, SUBSPACES, 8):
        left_high, left_low = split(left_ref, s)
        right_high, right_low = (left_high, left_low) if left_ref is right_ref else split(right_ref, s)
        total = total + lax.dot_general(
            jnp.concatenate([left_high, left_high, left_low], axis=1),
            jnp.concatenate([right_high, right_low, right_high], axis=1),
            (((1,), (1,)), ((), ())),
            preferred_element_type=jnp.float32,
        )
    return total


def own_kernel(levels_ref, surplus_ref, near_ref, block_ref, far_ref):
    grids = surplus_ref.shape[0]

    def mask(i, carry):
        tiles = owner_tiles(levels_ref, i)
        for k in range(TILES):
            at = tile_rows(i, k)
            near_ref[at, :] = jnp.where(tiles[k], cell_tile(surplus_ref, i, k, 0), 0.0)
            far_ref[at, :] = jnp.where(tiles[k], cell_tile(surplus_ref, i, k, 1), 0.0)
        return carry

    lax.fori_loop(0, grids, mask, 0)
    block_ref[...] = products(near_ref, near_ref, grids) + products(far_ref, far_ref, grids)


def own_products(levels, surplus):
    grids = surplus.shape[0]
    half = (grids * SUBSPACES, LANES)
    return pl.pallas_call(
        own_kernel,
        out_shape=(
            jax.ShapeDtypeStruct(half, jnp.float32),
            jax.ShapeDtypeStruct((grids, grids), jnp.float32),
        ),
        in_specs=[SMEM, VMEM],
        out_specs=(VMEM, VMEM),
        scratch_shapes=[pltpu.VMEM(half, jnp.float32)],
    )(levels, surplus)


def fold(block, cross, turned, second):
    zero = jnp.zeros_like(block)
    return jnp.concatenate(
        [
            jnp.where(second, zero, block),
            jnp.where(second, turned, cross),
            jnp.where(second, cross, turned),
            jnp.where(second, block, zero),
            jnp.zeros((block.shape[0], LANES - 4 * block.shape[0]), jnp.float32),
        ],
        axis=1,
    )


def cross_kernel(levels_ref, near_ref, block_ref, got_ref, parts_ref, full_ref, other_ref, head, sem):
    grids = block_ref.shape[0]
    fetch = pltpu.make_async_copy(got_ref.at[0:HEAD, :], head, sem)
    fetch.start()
    own = jnp.int32(HEAD)
    for i in range(grids):
        own = own + (levels_ref[0, i] + 1) * (levels_ref[1, i] + 1) * (levels_ref[2, i] + 1)
    fetch.wait()

    def unpack(i, start):
        rows, stop = positions(head, i, start)
        tiles = owner_tiles(head, i)
        for k in range(TILES):
            tile = packed_tile(got_ref, rows, k)
            other_ref[tile_rows(i, k), :] = jnp.where(tiles[k], tile, 0.0)
        return stop

    stop = lax.fori_loop(0, grids, unpack, jnp.int32(HEAD))
    full_ref[0] = (jnp.maximum(own, stop) > HEAD + ROOM).astype(jnp.int32)
    cross = products(near_ref, other_ref, grids)
    folded = fold(block_ref[...], cross, cross.T, lax.axis_index("grp") == 1)
    for k in range(parts_ref.shape[0]):
        parts_ref[k] = folded


def cross_products(levels, near, block, got, copies):
    grids = block.shape[0]
    return pl.pallas_call(
        cross_kernel,
        out_shape=(
            jax.ShapeDtypeStruct((copies, grids, LANES), jnp.float32),
            jax.ShapeDtypeStruct((1,), jnp.int32),
        ),
        in_specs=[SMEM, VMEM, VMEM, VMEM],
        out_specs=(VMEM, SMEM),
        scratch_shapes=[
            pltpu.VMEM((grids * SUBSPACES, LANES), jnp.float32),
            pltpu.SMEM((HEAD, LANES), jnp.float32),
            pltpu.SemaphoreType.DMA,
        ],
    )(levels, near, block, got)


def eliminate(parts_ref):
    number = 2 * parts_ref.shape[1]
    folded = parts_ref[0]
    for k in range(1, parts_ref.shape[0]):
        folded = folded + parts_ref[k]
    gram = jnp.concatenate([folded, pltpu.roll(folded, LANES - number, 1)], axis=0)
    rows = lax.broadcasted_iota(jnp.int32, gram.shape, 0)
    lanes = lax.broadcasted_iota(jnp.int32, gram.shape, 1)
    on_diagonal = rows == lanes
    diagonal = jnp.sum(jnp.where(on_diagonal, gram, 0.0), axis=1, keepdims=True) + 1e-06
    system = jnp.where(lanes < number, gram, 0.0) + jnp.where(on_diagonal, 0.1 * diagonal, 0.0)
    system = jnp.where(lanes == number, diagonal, system)
    for k in range(number):
        row = system[k : k + 1, :]
        column = jnp.broadcast_to(system[:, k : k + 1], system.shape)
        scaled = row * (1.0 / column[k : k + 1, :])
        system = system - jnp.where(rows == k, 0.0, column) * jnp.broadcast_to(scaled, system.shape)
    last = jnp.broadcast_to(system[:, number : number + 1], system.shape)
    solved = jnp.where(on_diagonal, last / system, 0.0)
    return jnp.broadcast_to(jnp.sum(solved, axis=1, keepdims=True), system.shape), on_diagonal


def solve_kernel(parts_ref, out_ref):
    solution_rows, on_diagonal = eliminate(parts_ref)
    out_ref[...] = jnp.sum(jnp.where(on_diagonal, solution_rows, 0.0), axis=0, keepdims=True)[:, : out_ref.shape[1]]


def solve_parts(parts):
    return pl.pallas_call(
        solve_kernel,
        out_shape=jax.ShapeDtypeStruct((1, 2 * parts.shape[1]), jnp.float32),
        in_specs=[VMEM],
        out_specs=VMEM,
    )(parts)


def finish_kernel(
    levels_ref,
    parts_ref,
    surplus_ref,
    got_near_ref,
    got_far_ref,
    updated_ref,
    out_ref,
    head,
    head_sem,
    weights,
    result,
    out_sems,
):
    grids = surplus_ref.shape[0]
    side = lax.axis_index("grp")
    fetch = pltpu.make_async_copy(got_near_ref.at[0:HEAD, :], head, head_sem)
    fetch.start()
    solution_rows, on_diagonal = eliminate(parts_ref)
    out_ref[...] = jnp.sum(jnp.where(on_diagonal, solution_rows, 0.0), axis=0, keepdims=True)[:, : out_ref.shape[1]]
    weights[...] = solution_rows
    fetch.wait()

    def add(i, carry):
        start, sums = carry
        rows, stop = positions(head, i, start)
        own_tiles = owner_tiles(levels_ref, i)
        other_tiles = owner_tiles(head, i)
        own = jnp.broadcast_to(weights[pl.ds(side * grids + i, 1), :], (8, LANES))
        other = jnp.broadcast_to(weights[pl.ds((1 - side) * grids + i, 1), :], (8, LANES))
        added = []
        for slot, got in ((0, got_near_ref), (1, got_far_ref)):
            for k in range(TILES):
                mine = jnp.where(own_tiles[k], cell_tile(surplus_ref, i, k, slot), 0.0)
                theirs = jnp.where(other_tiles[k], packed_tile(got, rows, k), 0.0)
                added.append(sums[slot * TILES + k] + own * mine + other * theirs)
        return stop, tuple(added)

    zero = jnp.zeros((8, LANES), jnp.float32)
    _, sums = lax.fori_loop(0, grids, add, (jnp.int32(HEAD), (zero,) * (2 * TILES)))

    def put(i, slot):
        rows = pl.ds(i * SUBSPACES, SUBSPACES)
        return pltpu.make_async_copy(result.at[slot, rows, :], updated_ref.at[i, :, half_lanes(slot)], out_sems.at[slot, i])

    def spread(i, carry):
        tiles = owner_tiles(levels_ref, i)
        for slot in range(2):
            for k in range(TILES):
                result[slot, tile_rows(i, k), :] = jnp.where(tiles[k], sums[slot * TILES + k], 0.0)
            put(i, slot).start()
        return carry

    lax.fori_loop(0, grids, spread, 0)
    for i in range(grids):
        put(i, 0).wait()
        put(i, 1).wait()


def finish(levels, parts, surplus, got_near, got_far):
    grids = surplus.shape[0]
    return pl.pallas_call(
        finish_kernel,
        out_shape=(
            jax.ShapeDtypeStruct(surplus.shape, jnp.float32),
            jax.ShapeDtypeStruct((1, 2 * grids), jnp.float32),
        ),
        in_specs=[SMEM, VMEM, VMEM, VMEM, VMEM],
        out_specs=(ANY, VMEM),
        scratch_shapes=[
            pltpu.SMEM((HEAD, LANES), jnp.float32),
            pltpu.SemaphoreType.DMA,
            pltpu.VMEM((2 * grids, LANES), jnp.float32),
            pltpu.VMEM((2, grids * SUBSPACES, LANES), jnp.float32),
            pltpu.SemaphoreType.DMA((2, grids)),
        ],
    )(levels, parts, surplus, got_near, got_far)


def owned(levels, count):
    indices = jnp.arange(count, dtype=jnp.int32)
    digits = jnp.stack([indices // 16, indices // 4 % 4, indices % 4])
    return jnp.all(digits[:, None] <= levels[:, :, None], axis=0).astype(jnp.float32)


def halves(levels, surplus):
    second = lax.axis_index("grp") == 1
    masked = surplus * owned(levels, SUBSPACES)[:, :, None]
    low, high = masked[:, :, :LANES], masked[:, :, LANES:]
    return jnp.where(second, high, low), jnp.where(second, low, high)


def dense_parts(levels, surplus, block, copies):
    near, far = halves(levels, surplus)
    cross = lax.dot_general(
        near,
        lax.ppermute(far, "grp", SWAP),
        (((1, 2), (1, 2)), ((), ())),
        precision=lax.Precision.HIGHEST,
        preferred_element_type=jnp.float32,
    )
    folded = fold(block, cross, cross.T, lax.axis_index("grp") == 1)
    return jnp.broadcast_to(folded, (copies, *folded.shape))


def dense_finish(levels, parts, surplus):
    grids = surplus.shape[0]
    second = lax.axis_index("grp") == 1
    near, far = halves(levels, surplus)
    got_near = lax.ppermute(far, "grp", SWAP)
    got_far = lax.ppermute(near, "grp", SWAP)
    coefficients = solve_parts(parts)
    start, stop = coefficients[0, :grids], coefficients[0, grids : 2 * grids]
    own = jnp.where(second, stop, start)[:, None, None]
    other = jnp.where(second, start, stop)[:, None, None]
    sum_near = jnp.sum(own * near + other * got_near, axis=0)
    sum_far = jnp.sum(own * far + other * got_far, axis=0)
    combined = jnp.concatenate(
        [jnp.where(second, sum_far, sum_near), jnp.where(second, sum_near, sum_far)], axis=1
    )
    return owned(levels, SUBSPACES)[:, :, None] * combined[None], coefficients


def exchanged(copies, axes):
    return lax.all_to_all(copies, axes, split_axis=0, concat_axis=0, tiled=True)


def whole(surplus, levels):
    levels = levels.T
    far = pack_far(levels, surplus)
    got_near = lax.ppermute(far, "grp", SWAP)
    near = pack_near(levels, surplus)
    got_far = lax.ppermute(near, "grp", SWAP)
    own, block = own_products(levels, surplus)
    parts, full = cross_products(levels, own, block, got_near, lax.axis_size(STAGES[0]))
    dense = full[0] > 0
    parts = lax.cond(
        dense, lambda: dense_parts(levels, surplus, block, parts.shape[0]), lambda: parts
    )
    for axes, following in zip(STAGES, STAGES[1:]):
        folded = jnp.sum(exchanged(parts, axes), axis=0)
        parts = jnp.broadcast_to(folded, (lax.axis_size(following), *folded.shape))
    parts = exchanged(parts, STAGES[-1])
    updated, coefficients = lax.cond(
        dense,
        lambda: dense_finish(levels, parts, surplus),
        lambda: tuple(finish(levels, parts, surplus, got_near, got_far)),
    )
    return updated, coefficients.reshape(-1)


def solution(mesh):
    torus = Mesh(
        mesh.devices.reshape(mesh.shape["grp"], 4, 2, 4, 2, 2, 2),
        ("grp", *DOM),
    )
    return jax.shard_map(
        whole,
        mesh=torus,
        in_specs=(P("grp", None, DOM), P("grp", None)),
        out_specs=(P("grp", None, DOM), P()),
        check_vma=False,
    )
```

```python
import jax
import jax.numpy as jnp
from jax import lax
from jax.experimental import pallas as pl
from jax.experimental.pallas import tpu as pltpu
from jax.sharding import Mesh
from jax.sharding import PartitionSpec as P

DOM = ("z", "y", "x_hi", "core")
STAGES = (("z",), ("y",), ("grp", "x_hi", "core"))
SWAP = ((0, 1), (1, 0))
LANES = 128
SUBSPACES = 64
TILES = 8
HEAD = 8
ROOM = 576
ROWS = HEAD + ROOM + 24
VMEM = pl.BlockSpec(memory_space=pltpu.VMEM)
SMEM = pl.BlockSpec(memory_space=pltpu.SMEM)
ANY = pl.BlockSpec(memory_space=pl.ANY)
HBM = pl.BlockSpec(memory_space=pltpu.HBM)


def positions(levels, i, start):
    l0, l1, l2 = (levels[d, i].astype(jnp.int32) for d in range(3))
    width = l2 + 1
    block = (l1 + 1) * width
    rows = []
    at = start
    for _ in range(4):
        base = jnp.minimum(at, HEAD + ROOM)
        rows += [base, base + width, base + 2 * width, base + 3 * width]
        at = at + block
    return rows, start + (l0 + 1) * block


def owner_tiles(levels, i):
    l0, l1, l2 = (levels[d, i].astype(jnp.int32) for d in range(3))
    row = lax.broadcasted_iota(jnp.int32, (8, LANES), 0)
    fits = (row & 3) <= l2
    return [fits & (k % 2 * 2 + (row >> 2) <= l1) & (k // 2 <= l0) for k in range(TILES)]


def tile_rows(i, k):
    return pl.ds(pl.multiple_of(i * SUBSPACES + k * 8, 8), 8)


def packed_tile(packed_ref, rows, k):
    row = lax.broadcasted_iota(jnp.int32, (8, LANES), 0)
    upper = packed_ref[pl.ds(rows[2 * k], 8), :]
    lower = packed_ref[pl.ds(rows[2 * k + 1] - 4, 8), :]
    return jnp.where(row < 4, upper, lower)


def half_lanes(slot):
    side = lax.axis_index("grp")
    return pl.ds(pl.multiple_of((1 - side if slot else side) * LANES, LANES), LANES)


def cell_tile(surplus_ref, i, k, slot):
    return surplus_ref[i, k * 8 : k * 8 + 8, half_lanes(slot)]


def store_packed(out_ref, rows, k, tile):
    out_ref[pl.ds(rows[2 * k], 4), :] = tile[0:4]
    out_ref[pl.ds(rows[2 * k + 1], 4), :] = tile[4:8]


def pack_far_kernel(levels_ref, surplus_ref, out_ref, held, sems):
    grids = surplus_ref.shape[0]

    def copy(i):
        rows = pl.ds(i * SUBSPACES, SUBSPACES)
        return pltpu.make_async_copy(surplus_ref.at[i, :, half_lanes(1)], held.at[rows, :], sems.at[i])

    for i in range(grids):
        copy(i).start()
    head = jnp.zeros((HEAD, LANES), jnp.float32)
    row = lax.broadcasted_iota(jnp.int32, head.shape, 0)
    lane = lax.broadcasted_iota(jnp.int32, head.shape, 1)
    for d in range(3):
        for i in range(grids):
            head = jnp.where((row == d) & (lane == i), levels_ref[d, i].astype(jnp.float32), head)
    out_ref[0:HEAD, :] = head

    def pack(i, start):
        copy(i).wait()
        rows, stop = positions(levels_ref, i, start)
        for k in range(TILES):
            store_packed(out_ref, rows, k, held[tile_rows(i, k), :])
        return stop

    lax.fori_loop(0, grids, pack, jnp.int32(HEAD))


def pack_far(levels, surplus):
    grids = surplus.shape[0]
    return pl.pallas_call(
        pack_far_kernel,
        out_shape=jax.ShapeDtypeStruct((ROWS, LANES), jnp.float32),
        in_specs=[SMEM, ANY],
        out_specs=VMEM,
        scratch_shapes=[
            pltpu.VMEM((grids * SUBSPACES, LANES), jnp.float32),
            pltpu.SemaphoreType.DMA((grids,)),
        ],
    )(levels, surplus)


def pack_near_kernel(levels_ref, surplus_ref, out_ref):
    grids = surplus_ref.shape[0]
    out_ref[0:HEAD, :] = jnp.zeros((HEAD, LANES), jnp.float32)

    def pack(i, start):
        rows, stop = positions(levels_ref, i, start)
        for k in range(TILES):
            store_packed(out_ref, rows, k, cell_tile(surplus_ref, i, k, 0))
        return stop

    lax.fori_loop(0, grids, pack, jnp.int32(HEAD))


def pack_near(levels, surplus):
    return pl.pallas_call(
        pack_near_kernel,
        out_shape=jax.ShapeDtypeStruct((ROWS, LANES), jnp.float32),
        in_specs=[SMEM, VMEM],
        out_specs=VMEM,
    )(levels, surplus)


def split(ref, s, grids):
    rows = [ref[pl.ds(s + k, grids, stride=SUBSPACES), :] for k in range(8)]
    rows = jnp.concatenate(rows, axis=1)
    high = rows.astype(jnp.bfloat16)
    return high, (rows - high.astype(jnp.float32)).astype(jnp.bfloat16)


def inner(left, right):
    return lax.dot_general(
        jnp.concatenate([left[0], left[0], left[1]], axis=1),
        jnp.concatenate([right[0], right[1], right[0]], axis=1),
        (((1,), (1,)), ((), ())),
        preferred_element_type=jnp.float32,
    )


def own_kernel(levels_ref, surplus_ref, high_ref, low_ref, block_ref, near_ref, far_ref):
    grids = surplus_ref.shape[0]

    def mask(i, carry):
        tiles = owner_tiles(levels_ref, i)
        for k in range(TILES):
            at = tile_rows(i, k)
            near_ref[at, :] = jnp.where(tiles[k], cell_tile(surplus_ref, i, k, 0), 0.0)
            far_ref[at, :] = jnp.where(tiles[k], cell_tile(surplus_ref, i, k, 1), 0.0)
        return carry

    lax.fori_loop(0, grids, mask, 0)
    total = jnp.zeros((grids, grids), jnp.float32)
    for s in range(0, SUBSPACES, 8):
        near = split(near_ref, s, grids)
        far = split(far_ref, s, grids)
        high_ref[:, s * LANES : (s + 8) * LANES] = near[0]
        low_ref[:, s * LANES : (s + 8) * LANES] = near[1]
        total = total + inner(near, near) + inner(far, far)
    block_ref[...] = total


def own_products(levels, surplus):
    grids = surplus.shape[0]
    part = jax.ShapeDtypeStruct((grids, SUBSPACES * LANES), jnp.bfloat16)
    half = pltpu.VMEM((grids * SUBSPACES, LANES), jnp.float32)
    return pl.pallas_call(
        own_kernel,
        out_shape=(part, part, jax.ShapeDtypeStruct((grids, grids), jnp.float32)),
        in_specs=[SMEM, VMEM],
        out_specs=(VMEM, VMEM, VMEM),
        scratch_shapes=[half, half],
    )(levels, surplus)


def fold(block, cross, turned, second):
    zero = jnp.zeros_like(block)
    return jnp.concatenate(
        [
            jnp.where(second, zero, block),
            jnp.where(second, turned, cross),
            jnp.where(second, cross, turned),
            jnp.where(second, block, zero),
            jnp.zeros((block.shape[0], LANES - 4 * block.shape[0]), jnp.float32),
        ],
        axis=1,
    )


def cross_kernel(
    levels_ref, high_ref, low_ref, block_ref, got_ref, parts_ref, full_ref, other_ref, high, low, head, sems
):
    grids = block_ref.shape[0]
    fetch = pltpu.make_async_copy(got_ref.at[0:HEAD, :], head, sems.at[0])
    fetch_high = pltpu.make_async_copy(high_ref, high, sems.at[1])
    fetch_low = pltpu.make_async_copy(low_ref, low, sems.at[2])
    fetch.start()
    fetch_high.start()
    fetch_low.start()
    own = jnp.int32(HEAD)
    for i in range(grids):
        own = own + (levels_ref[0, i] + 1) * (levels_ref[1, i] + 1) * (levels_ref[2, i] + 1)
    fetch.wait()

    def unpack(i, start):
        rows, stop = positions(head, i, start)
        tiles = owner_tiles(head, i)
        for k in range(TILES):
            tile = packed_tile(got_ref, rows, k)
            other_ref[tile_rows(i, k), :] = jnp.where(tiles[k], tile, 0.0)
        return stop

    stop = lax.fori_loop(0, grids, unpack, jnp.int32(HEAD))
    full_ref[0] = (jnp.maximum(own, stop) > HEAD + ROOM).astype(jnp.int32)
    fetch_high.wait()
    fetch_low.wait()
    cross = jnp.zeros((grids, grids), jnp.float32)
    for s in range(0, SUBSPACES, 8):
        at = slice(s * LANES, (s + 8) * LANES)
        cross = cross + inner((high[:, at], low[:, at]), split(other_ref, s, grids))
    folded = fold(block_ref[...], cross, cross.T, lax.axis_index("grp") == 1)
    for k in range(parts_ref.shape[0]):
        parts_ref[k] = folded


def cross_products(levels, high, low, block, got, copies):
    grids = block.shape[0]
    return pl.pallas_call(
        cross_kernel,
        out_shape=(
            jax.ShapeDtypeStruct((copies, grids, LANES), jnp.float32),
            jax.ShapeDtypeStruct((1,), jnp.int32),
        ),
        in_specs=[SMEM, HBM, HBM, VMEM, VMEM],
        out_specs=(VMEM, SMEM),
        scratch_shapes=[
            pltpu.VMEM((grids * SUBSPACES, LANES), jnp.float32),
            pltpu.VMEM(high.shape, high.dtype),
            pltpu.VMEM(low.shape, low.dtype),
            pltpu.SMEM((HEAD, LANES), jnp.float32),
            pltpu.SemaphoreType.DMA((3,)),
        ],
    )(levels, high, low, block, got)


def eliminate(parts_ref):
    number = 2 * parts_ref.shape[1]
    folded = parts_ref[0]
    for k in range(1, parts_ref.shape[0]):
        folded = folded + parts_ref[k]
    gram = jnp.concatenate([folded, pltpu.roll(folded, LANES - number, 1)], axis=0)
    rows = lax.broadcasted_iota(jnp.int32, gram.shape, 0)
    lanes = lax.broadcasted_iota(jnp.int32, gram.shape, 1)
    on_diagonal = rows == lanes
    diagonal = jnp.sum(jnp.where(on_diagonal, gram, 0.0), axis=1, keepdims=True) + 1e-06
    system = jnp.where(lanes < number, gram, 0.0) + jnp.where(on_diagonal, 0.1 * diagonal, 0.0)
    system = jnp.where(lanes == number, diagonal, system)
    for first in range(0, number, 8):
        columns = [
            jnp.broadcast_to(system[:, k : k + 1], system.shape) for k in range(first, first + 8)
        ]
        for j in range(8):
            k = first + j
            inverse = 1.0 / columns[j][k : k + 1, :]
            column = jnp.where(rows == k, 0.0, columns[j])
            system = system - column * (system[k : k + 1, :] * inverse)
            for q in range(j + 1, 8):
                scale = columns[j][first + q : first + q + 1, :] * inverse
                columns[q] = columns[q] - column * scale
    last = jnp.broadcast_to(system[:, number : number + 1], system.shape)
    solved = jnp.where(on_diagonal, last / system, 0.0)
    return jnp.broadcast_to(jnp.sum(solved, axis=1, keepdims=True), system.shape), on_diagonal


def solve_kernel(parts_ref, out_ref):
    solution_rows, on_diagonal = eliminate(parts_ref)
    out_ref[...] = jnp.sum(jnp.where(on_diagonal, solution_rows, 0.0), axis=0, keepdims=True)[:, : out_ref.shape[1]]


def solve_parts(parts):
    return pl.pallas_call(
        solve_kernel,
        out_shape=jax.ShapeDtypeStruct((1, 2 * parts.shape[1]), jnp.float32),
        in_specs=[VMEM],
        out_specs=VMEM,
    )(parts)


def finish_kernel(
    levels_ref,
    parts_ref,
    surplus_ref,
    got_near_ref,
    got_far_ref,
    updated_ref,
    out_ref,
    head,
    head_sem,
    weights,
    result,
    out_sems,
):
    grids = surplus_ref.shape[0]
    side = lax.axis_index("grp")
    fetch = pltpu.make_async_copy(got_near_ref.at[0:HEAD, :], head, head_sem)
    fetch.start()
    solution_rows, on_diagonal = eliminate(parts_ref)
    out_ref[...] = jnp.sum(jnp.where(on_diagonal, solution_rows, 0.0), axis=0, keepdims=True)[:, : out_ref.shape[1]]
    weights[...] = solution_rows
    fetch.wait()

    def add(i, carry):
        start, sums = carry
        rows, stop = positions(head, i, start)
        own_tiles = owner_tiles(levels_ref, i)
        other_tiles = owner_tiles(head, i)
        own = jnp.broadcast_to(weights[pl.ds(side * grids + i, 1), :], (8, LANES))
        other = jnp.broadcast_to(weights[pl.ds((1 - side) * grids + i, 1), :], (8, LANES))
        added = []
        for slot, got in ((0, got_near_ref), (1, got_far_ref)):
            for k in range(TILES):
                mine = jnp.where(own_tiles[k], cell_tile(surplus_ref, i, k, slot), 0.0)
                theirs = jnp.where(other_tiles[k], packed_tile(got, rows, k), 0.0)
                added.append(sums[slot * TILES + k] + own * mine + other * theirs)
        return stop, tuple(added)

    zero = jnp.zeros((8, LANES), jnp.float32)
    _, sums = lax.fori_loop(0, grids, add, (jnp.int32(HEAD), (zero,) * (2 * TILES)))

    def put(i, slot):
        rows = pl.ds(i * SUBSPACES, SUBSPACES)
        return pltpu.make_async_copy(result.at[slot, rows, :], updated_ref.at[i, :, half_lanes(slot)], out_sems.at[slot, i])

    def spread(i, carry):
        tiles = owner_tiles(levels_ref, i)
        for slot in range(2):
            for k in range(TILES):
                result[slot, tile_rows(i, k), :] = jnp.where(tiles[k], sums[slot * TILES + k], 0.0)
            put(i, slot).start()
        return carry

    lax.fori_loop(0, grids, spread, 0)
    for i in range(grids):
        put(i, 0).wait()
        put(i, 1).wait()


def finish(levels, parts, surplus, got_near, got_far):
    grids = surplus.shape[0]
    return pl.pallas_call(
        finish_kernel,
        out_shape=(
            jax.ShapeDtypeStruct(surplus.shape, jnp.float32),
            jax.ShapeDtypeStruct((1, 2 * grids), jnp.float32),
        ),
        in_specs=[SMEM, VMEM, VMEM, VMEM, VMEM],
        out_specs=(ANY, VMEM),
        scratch_shapes=[
            pltpu.SMEM((HEAD, LANES), jnp.float32),
            pltpu.SemaphoreType.DMA,
            pltpu.VMEM((2 * grids, LANES), jnp.float32),
            pltpu.VMEM((2, grids * SUBSPACES, LANES), jnp.float32),
            pltpu.SemaphoreType.DMA((2, grids)),
        ],
    )(levels, parts, surplus, got_near, got_far)


def owned(levels, count):
    indices = jnp.arange(count, dtype=jnp.int32)
    digits = jnp.stack([indices // 16, indices // 4 % 4, indices % 4])
    return jnp.all(digits[:, None] <= levels[:, :, None], axis=0).astype(jnp.float32)


def halves(levels, surplus):
    second = lax.axis_index("grp") == 1
    masked = surplus * owned(levels, SUBSPACES)[:, :, None]
    low, high = masked[:, :, :LANES], masked[:, :, LANES:]
    return jnp.where(second, high, low), jnp.where(second, low, high)


def dense_parts(levels, surplus, block, copies):
    near, far = halves(levels, surplus)
    cross = lax.dot_general(
        near,
        lax.ppermute(far, "grp", SWAP),
        (((1, 2), (1, 2)), ((), ())),
        precision=lax.Precision.HIGHEST,
        preferred_element_type=jnp.float32,
    )
    folded = fold(block, cross, cross.T, lax.axis_index("grp") == 1)
    return jnp.broadcast_to(folded, (copies, *folded.shape))


def dense_finish(levels, parts, surplus):
    grids = surplus.shape[0]
    second = lax.axis_index("grp") == 1
    near, far = halves(levels, surplus)
    got_near = lax.ppermute(far, "grp", SWAP)
    got_far = lax.ppermute(near, "grp", SWAP)
    coefficients = solve_parts(parts)
    start, stop = coefficients[0, :grids], coefficients[0, grids : 2 * grids]
    own = jnp.where(second, stop, start)[:, None, None]
    other = jnp.where(second, start, stop)[:, None, None]
    sum_near = jnp.sum(own * near + other * got_near, axis=0)
    sum_far = jnp.sum(own * far + other * got_far, axis=0)
    combined = jnp.concatenate(
        [jnp.where(second, sum_far, sum_near), jnp.where(second, sum_near, sum_far)], axis=1
    )
    return owned(levels, SUBSPACES)[:, :, None] * combined[None], coefficients


def exchanged(copies, axes):
    return lax.all_to_all(copies, axes, split_axis=0, concat_axis=0, tiled=True)


def whole(surplus, levels):
    levels = levels.T
    far = pack_far(levels, surplus)
    got_near = lax.ppermute(far, "grp", SWAP)
    near = pack_near(levels, surplus)
    got_far = lax.ppermute(near, "grp", SWAP)
    high, low, block = own_products(levels, surplus)
    parts, full = cross_products(levels, high, low, block, got_near, lax.axis_size(STAGES[0]))
    dense = full[0] > 0
    parts = lax.cond(
        dense, lambda: dense_parts(levels, surplus, block, parts.shape[0]), lambda: parts
    )
    for axes, following in zip(STAGES, STAGES[1:]):
        folded = jnp.sum(exchanged(parts, axes), axis=0)
        parts = jnp.broadcast_to(folded, (lax.axis_size(following), *folded.shape))
    parts = exchanged(parts, STAGES[-1])
    updated, coefficients = lax.cond(
        dense,
        lambda: dense_finish(levels, parts, surplus),
        lambda: tuple(finish(levels, parts, surplus, got_near, got_far)),
    )
    return updated, coefficients.reshape(-1)


def solution(mesh):
    torus = Mesh(
        mesh.devices.reshape(mesh.shape["grp"], 8, 8, 2, 2),
        ("grp", *DOM),
    )
    return jax.shard_map(
        whole,
        mesh=torus,
        in_specs=(P("grp", None, DOM), P("grp", None)),
        out_specs=(P("grp", None, DOM), P()),
        check_vma=False,
    )
```

```python
import jax
import jax.numpy as jnp
from jax import lax
from jax.experimental import pallas as pl
from jax.experimental.pallas import tpu as pltpu
from jax.sharding import Mesh
from jax.sharding import PartitionSpec as P

DOM = ("z", "y", "x_hi", "core")
STAGES = (("z",), ("y",), ("grp", "x_hi", "core"))
SWAP = ((0, 1), (1, 0))
LANES = 128
SUBSPACES = 64
TILES = 8
HEAD = 8
ROOM = 576
ROWS = HEAD + ROOM + 24
VMEM = pl.BlockSpec(memory_space=pltpu.VMEM)
SMEM = pl.BlockSpec(memory_space=pltpu.SMEM)
ANY = pl.BlockSpec(memory_space=pl.ANY)
HBM = pl.BlockSpec(memory_space=pltpu.HBM)


def positions(levels, i, start):
    l0, l1, l2 = (levels[d, i].astype(jnp.int32) for d in range(3))
    width = l2 + 1
    block = (l1 + 1) * width
    rows = []
    at = start
    for _ in range(4):
        base = jnp.minimum(at, HEAD + ROOM)
        rows += [base, base + width, base + 2 * width, base + 3 * width]
        at = at + block
    return rows, start + (l0 + 1) * block


def owner_tiles(levels, i):
    l0, l1, l2 = (levels[d, i].astype(jnp.int32) for d in range(3))
    row = lax.broadcasted_iota(jnp.int32, (8, LANES), 0)
    fits = (row & 3) <= l2
    return [fits & (k % 2 * 2 + (row >> 2) <= l1) & (k // 2 <= l0) for k in range(TILES)]


def tile_rows(i, k):
    return pl.ds(pl.multiple_of(i * SUBSPACES + k * 8, 8), 8)


def packed_tile(packed_ref, rows, k):
    row = lax.broadcasted_iota(jnp.int32, (8, LANES), 0)
    upper = packed_ref[pl.ds(rows[2 * k], 8), :]
    lower = packed_ref[pl.ds(rows[2 * k + 1] - 4, 8), :]
    return jnp.where(row < 4, upper, lower)


def half_lanes(slot):
    side = lax.axis_index("grp")
    return pl.ds(pl.multiple_of((1 - side if slot else side) * LANES, LANES), LANES)


def cell_tile(surplus_ref, i, k, slot):
    return surplus_ref[i, k * 8 : k * 8 + 8, half_lanes(slot)]


def store_packed(out_ref, rows, k, tile):
    out_ref[pl.ds(rows[2 * k], 4), :] = tile[0:4]
    out_ref[pl.ds(rows[2 * k + 1], 4), :] = tile[4:8]


def pack_far_kernel(levels_ref, surplus_ref, out_ref, held, sems):
    grids = surplus_ref.shape[0]

    def copy(i):
        rows = pl.ds(i * SUBSPACES, SUBSPACES)
        return pltpu.make_async_copy(surplus_ref.at[i, :, half_lanes(1)], held.at[rows, :], sems.at[i])

    for i in range(grids):
        copy(i).start()
    head = jnp.zeros((HEAD, LANES), jnp.float32)
    row = lax.broadcasted_iota(jnp.int32, head.shape, 0)
    lane = lax.broadcasted_iota(jnp.int32, head.shape, 1)
    for d in range(3):
        for i in range(grids):
            head = jnp.where((row == d) & (lane == i), levels_ref[d, i].astype(jnp.float32), head)
    out_ref[0:HEAD, :] = head

    def pack(i, start):
        copy(i).wait()
        rows, stop = positions(levels_ref, i, start)
        for k in range(TILES):
            store_packed(out_ref, rows, k, held[tile_rows(i, k), :])
        return stop

    lax.fori_loop(0, grids, pack, jnp.int32(HEAD))


def pack_far(levels, surplus):
    grids = surplus.shape[0]
    return pl.pallas_call(
        pack_far_kernel,
        out_shape=jax.ShapeDtypeStruct((ROWS, LANES), jnp.float32),
        in_specs=[SMEM, ANY],
        out_specs=VMEM,
        scratch_shapes=[
            pltpu.VMEM((grids * SUBSPACES, LANES), jnp.float32),
            pltpu.SemaphoreType.DMA((grids,)),
        ],
    )(levels, surplus)


def pack_near_kernel(levels_ref, surplus_ref, out_ref):
    grids = surplus_ref.shape[0]
    out_ref[0:HEAD, :] = jnp.zeros((HEAD, LANES), jnp.float32)

    def pack(i, start):
        rows, stop = positions(levels_ref, i, start)
        for k in range(TILES):
            store_packed(out_ref, rows, k, cell_tile(surplus_ref, i, k, 0))
        return stop

    lax.fori_loop(0, grids, pack, jnp.int32(HEAD))


def pack_near(levels, surplus):
    return pl.pallas_call(
        pack_near_kernel,
        out_shape=jax.ShapeDtypeStruct((ROWS, LANES), jnp.float32),
        in_specs=[SMEM, VMEM],
        out_specs=VMEM,
    )(levels, surplus)


def split(ref, s, grids):
    rows = [ref[pl.ds(s + k, grids, stride=SUBSPACES), :] for k in range(8)]
    rows = jnp.concatenate(rows, axis=1)
    high = rows.astype(jnp.bfloat16)
    return high, (rows - high.astype(jnp.float32)).astype(jnp.bfloat16)


def inner(left, right):
    return lax.dot_general(
        jnp.concatenate([left[0], left[0], left[1]], axis=1),
        jnp.concatenate([right[0], right[1], right[0]], axis=1),
        (((1,), (1,)), ((), ())),
        preferred_element_type=jnp.float32,
    )


def own_kernel(levels_ref, surplus_ref, high_ref, low_ref, block_ref, near_ref, far_ref):
    grids = surplus_ref.shape[0]

    def mask(i, carry):
        tiles = owner_tiles(levels_ref, i)
        for k in range(TILES):
            at = tile_rows(i, k)
            near_ref[at, :] = jnp.where(tiles[k], cell_tile(surplus_ref, i, k, 0), 0.0)
            far_ref[at, :] = jnp.where(tiles[k], cell_tile(surplus_ref, i, k, 1), 0.0)
        return carry

    lax.fori_loop(0, grids, mask, 0)
    total = jnp.zeros((grids, grids), jnp.float32)
    for s in range(0, SUBSPACES, 8):
        near = split(near_ref, s, grids)
        far = split(far_ref, s, grids)
        high_ref[:, s * LANES : (s + 8) * LANES] = near[0]
        low_ref[:, s * LANES : (s + 8) * LANES] = near[1]
        total = total + inner(near, near) + inner(far, far)
    block_ref[...] = total


def own_products(levels, surplus):
    grids = surplus.shape[0]
    part = jax.ShapeDtypeStruct((grids, SUBSPACES * LANES), jnp.bfloat16)
    half = pltpu.VMEM((grids * SUBSPACES, LANES), jnp.float32)
    return pl.pallas_call(
        own_kernel,
        out_shape=(part, part, jax.ShapeDtypeStruct((grids, grids), jnp.float32)),
        in_specs=[SMEM, VMEM],
        out_specs=(VMEM, VMEM, VMEM),
        scratch_shapes=[half, half],
    )(levels, surplus)


def fold(block, cross):
    grids = block.shape[0]
    strips = range(0, grids, 8)
    pieces = [block[r : r + 8, r:] for r in strips] + [cross[r : r + 8, :] for r in strips]
    used = sum(piece.shape[1] for piece in pieces)
    return jnp.concatenate([*pieces, jnp.zeros((8, LANES - used), jnp.float32)], axis=1)


def unfold(first, last, grids):
    def upper(folded):
        strips, at = [], 0
        for r in range(0, grids, 8):
            strip = folded[:, at : at + grids - r]
            strips.append(jnp.concatenate([jnp.zeros((8, r), jnp.float32), strip], axis=1) if r else strip)
            at += grids - r
        return jnp.concatenate(strips, axis=0), at

    top, at = upper(first)
    low, _ = upper(last)
    both = first + last
    cross = jnp.concatenate(
        [both[:, at + n * grids : at + (n + 1) * grids] for n in range(grids // 8)], axis=0
    )
    half = jnp.concatenate(
        [jnp.concatenate([top, cross], axis=1), jnp.concatenate([jnp.zeros_like(low), low], axis=1)], axis=0
    )
    rows = lax.broadcasted_iota(jnp.int32, half.shape, 0) >> 3
    columns = lax.broadcasted_iota(jnp.int32, half.shape, 1) >> 3
    gram = jnp.where(rows <= columns, half, half.T)
    return jnp.concatenate([gram, jnp.zeros((2 * grids, LANES - 2 * grids), jnp.float32)], axis=1)


def cross_kernel(
    levels_ref, high_ref, low_ref, block_ref, got_ref, parts_ref, full_ref, other_ref, high, low, head, sems
):
    grids = block_ref.shape[0]
    fetch = pltpu.make_async_copy(got_ref.at[0:HEAD, :], head, sems.at[0])
    fetch_high = pltpu.make_async_copy(high_ref, high, sems.at[1])
    fetch_low = pltpu.make_async_copy(low_ref, low, sems.at[2])
    fetch.start()
    fetch_high.start()
    fetch_low.start()
    own = jnp.int32(HEAD)
    for i in range(grids):
        own = own + (levels_ref[0, i] + 1) * (levels_ref[1, i] + 1) * (levels_ref[2, i] + 1)
    fetch.wait()

    def unpack(i, start):
        rows, stop = positions(head, i, start)
        tiles = owner_tiles(head, i)
        for k in range(TILES):
            tile = packed_tile(got_ref, rows, k)
            other_ref[tile_rows(i, k), :] = jnp.where(tiles[k], tile, 0.0)
        return stop

    stop = lax.fori_loop(0, grids, unpack, jnp.int32(HEAD))
    full_ref[0] = (jnp.maximum(own, stop) > HEAD + ROOM).astype(jnp.int32)
    fetch_high.wait()
    fetch_low.wait()
    cross = jnp.zeros((grids, grids), jnp.float32)
    for s in range(0, SUBSPACES, 8):
        at = slice(s * LANES, (s + 8) * LANES)
        cross = cross + inner((high[:, at], low[:, at]), split(other_ref, s, grids))
    folded = fold(block_ref[...], jnp.where(lax.axis_index("grp") == 1, cross.T, cross))
    for k in range(parts_ref.shape[0]):
        parts_ref[k] = folded


def cross_products(levels, high, low, block, got, copies):
    grids = block.shape[0]
    return pl.pallas_call(
        cross_kernel,
        out_shape=(
            jax.ShapeDtypeStruct((copies, 8, LANES), jnp.float32),
            jax.ShapeDtypeStruct((1,), jnp.int32),
        ),
        in_specs=[SMEM, HBM, HBM, VMEM, VMEM],
        out_specs=(VMEM, SMEM),
        scratch_shapes=[
            pltpu.VMEM((grids * SUBSPACES, LANES), jnp.float32),
            pltpu.VMEM(high.shape, high.dtype),
            pltpu.VMEM(low.shape, low.dtype),
            pltpu.SMEM((HEAD, LANES), jnp.float32),
            pltpu.SemaphoreType.DMA((3,)),
        ],
    )(levels, high, low, block, got)


def eliminate(parts_ref, grids):
    number = 2 * grids
    senders = parts_ref.shape[0] // 2
    first, last = parts_ref[0], parts_ref[senders]
    for k in range(1, senders):
        first = first + parts_ref[k]
        last = last + parts_ref[senders + k]
    gram = unfold(first, last, grids)
    rows = lax.broadcasted_iota(jnp.int32, gram.shape, 0)
    lanes = lax.broadcasted_iota(jnp.int32, gram.shape, 1)
    on_diagonal = rows == lanes
    diagonal = jnp.sum(jnp.where(on_diagonal, gram, 0.0), axis=1, keepdims=True) + 1e-06
    system = gram + jnp.where(on_diagonal, 0.1 * diagonal, 0.0)
    system = jnp.where(lanes == number, diagonal, system)
    for first in range(0, number, 8):
        columns = [
            jnp.broadcast_to(system[:, k : k + 1], system.shape) for k in range(first, first + 8)
        ]
        for j in range(8):
            k = first + j
            inverse = 1.0 / columns[j][k : k + 1, :]
            column = jnp.where(rows == k, 0.0, columns[j])
            system = system - column * (system[k : k + 1, :] * inverse)
            for q in range(j + 1, 8):
                scale = columns[j][first + q : first + q + 1, :] * inverse
                columns[q] = columns[q] - column * scale
    last = jnp.broadcast_to(system[:, number : number + 1], system.shape)
    solved = jnp.where(on_diagonal, last / system, 0.0)
    return jnp.broadcast_to(jnp.sum(solved, axis=1, keepdims=True), system.shape), on_diagonal


def solve_kernel(parts_ref, out_ref):
    solution_rows, on_diagonal = eliminate(parts_ref, out_ref.shape[1] // 2)
    out_ref[...] = jnp.sum(jnp.where(on_diagonal, solution_rows, 0.0), axis=0, keepdims=True)[:, : out_ref.shape[1]]


def solve_parts(parts, grids):
    return pl.pallas_call(
        solve_kernel,
        out_shape=jax.ShapeDtypeStruct((1, 2 * grids), jnp.float32),
        in_specs=[VMEM],
        out_specs=VMEM,
    )(parts)


def finish_kernel(
    levels_ref,
    parts_ref,
    surplus_ref,
    got_near_ref,
    got_far_ref,
    updated_ref,
    out_ref,
    head,
    head_sem,
    weights,
    result,
    out_sems,
):
    grids = surplus_ref.shape[0]
    side = lax.axis_index("grp")
    fetch = pltpu.make_async_copy(got_near_ref.at[0:HEAD, :], head, head_sem)
    fetch.start()
    solution_rows, on_diagonal = eliminate(parts_ref, grids)
    out_ref[...] = jnp.sum(jnp.where(on_diagonal, solution_rows, 0.0), axis=0, keepdims=True)[:, : out_ref.shape[1]]
    weights[...] = solution_rows
    fetch.wait()

    def add(i, carry):
        start, sums = carry
        rows, stop = positions(head, i, start)
        own_tiles = owner_tiles(levels_ref, i)
        other_tiles = owner_tiles(head, i)
        own = jnp.broadcast_to(weights[pl.ds(side * grids + i, 1), :], (8, LANES))
        other = jnp.broadcast_to(weights[pl.ds((1 - side) * grids + i, 1), :], (8, LANES))
        added = []
        for slot, got in ((0, got_near_ref), (1, got_far_ref)):
            for k in range(TILES):
                mine = jnp.where(own_tiles[k], cell_tile(surplus_ref, i, k, slot), 0.0)
                theirs = jnp.where(other_tiles[k], packed_tile(got, rows, k), 0.0)
                added.append(sums[slot * TILES + k] + own * mine + other * theirs)
        return stop, tuple(added)

    zero = jnp.zeros((8, LANES), jnp.float32)
    _, sums = lax.fori_loop(0, grids, add, (jnp.int32(HEAD), (zero,) * (2 * TILES)))

    def put(i, slot):
        rows = pl.ds(i * SUBSPACES, SUBSPACES)
        return pltpu.make_async_copy(result.at[slot, rows, :], updated_ref.at[i, :, half_lanes(slot)], out_sems.at[slot, i])

    def spread(i, carry):
        tiles = owner_tiles(levels_ref, i)
        for slot in range(2):
            for k in range(TILES):
                result[slot, tile_rows(i, k), :] = jnp.where(tiles[k], sums[slot * TILES + k], 0.0)
            put(i, slot).start()
        return carry

    lax.fori_loop(0, grids, spread, 0)
    for i in range(grids):
        put(i, 0).wait()
        put(i, 1).wait()


def finish(levels, parts, surplus, got_near, got_far):
    grids = surplus.shape[0]
    return pl.pallas_call(
        finish_kernel,
        out_shape=(
            jax.ShapeDtypeStruct(surplus.shape, jnp.float32),
            jax.ShapeDtypeStruct((1, 2 * grids), jnp.float32),
        ),
        in_specs=[SMEM, VMEM, VMEM, VMEM, VMEM],
        out_specs=(ANY, VMEM),
        scratch_shapes=[
            pltpu.SMEM((HEAD, LANES), jnp.float32),
            pltpu.SemaphoreType.DMA,
            pltpu.VMEM((2 * grids, LANES), jnp.float32),
            pltpu.VMEM((2, grids * SUBSPACES, LANES), jnp.float32),
            pltpu.SemaphoreType.DMA((2, grids)),
        ],
    )(levels, parts, surplus, got_near, got_far)


def owned(levels, count):
    indices = jnp.arange(count, dtype=jnp.int32)
    digits = jnp.stack([indices // 16, indices // 4 % 4, indices % 4])
    return jnp.all(digits[:, None] <= levels[:, :, None], axis=0).astype(jnp.float32)


def halves(levels, surplus):
    second = lax.axis_index("grp") == 1
    masked = surplus * owned(levels, SUBSPACES)[:, :, None]
    low, high = masked[:, :, :LANES], masked[:, :, LANES:]
    return jnp.where(second, high, low), jnp.where(second, low, high)


def dense_finish(levels, surplus):
    grids = surplus.shape[0]
    second = lax.axis_index("grp") == 1
    near, far = halves(levels, surplus)
    got_near = lax.ppermute(far, "grp", SWAP)
    got_far = lax.ppermute(near, "grp", SWAP)

    def products(left, right):
        return lax.dot_general(
            left,
            right,
            (((1, 2), (1, 2)), ((), ())),
            precision=lax.Precision.HIGHEST,
            preferred_element_type=jnp.float32,
        )

    cross = products(near, got_near)
    own = products(near, near) + products(far, far)
    folded = fold(own, jnp.where(second, cross.T, cross))
    pair = jnp.stack([jnp.where(second, 0.0, folded), jnp.where(second, folded, 0.0)])
    for axis in ("grp", *DOM):
        pair = lax.psum(pair, axis)
    coefficients = solve_parts(pair, grids)
    start, stop = coefficients[0, :grids], coefficients[0, grids:]
    own = jnp.where(second, stop, start)[:, None, None]
    other = jnp.where(second, start, stop)[:, None, None]
    sum_near = jnp.sum(own * near + other * got_near, axis=0)
    sum_far = jnp.sum(own * far + other * got_far, axis=0)
    combined = jnp.concatenate(
        [jnp.where(second, sum_far, sum_near), jnp.where(second, sum_near, sum_far)], axis=1
    )
    return owned(levels, SUBSPACES)[:, :, None] * combined[None], coefficients


def exchanged(copies, axes):
    return lax.all_to_all(copies, axes, split_axis=0, concat_axis=0, tiled=True)


def whole(surplus, levels):
    levels = levels.T
    far = pack_far(levels, surplus)
    got_near = lax.ppermute(far, "grp", SWAP)
    near = pack_near(levels, surplus)
    got_far = lax.ppermute(near, "grp", SWAP)
    high, low, block = own_products(levels, surplus)
    parts, full = cross_products(levels, high, low, block, got_near, lax.axis_size(STAGES[0]))
    for axes, following in zip(STAGES, STAGES[1:]):
        folded = jnp.sum(exchanged(parts, axes), axis=0)
        parts = jnp.broadcast_to(folded, (lax.axis_size(following), *folded.shape))
    parts = exchanged(parts, STAGES[-1])
    updated, coefficients = lax.cond(
        full[0] > 0,
        lambda: dense_finish(levels, surplus),
        lambda: tuple(finish(levels, parts, surplus, got_near, got_far)),
    )
    return updated, coefficients.reshape(-1)


def solution(mesh):
    torus = Mesh(
        mesh.devices.reshape(mesh.shape["grp"], 8, 8, 2, 2),
        ("grp", *DOM),
    )
    return jax.shard_map(
        whole,
        mesh=torus,
        in_specs=(P("grp", None, DOM), P("grp", None)),
        out_specs=(P("grp", None, DOM), P()),
        check_vma=False,
    )
```

```python
import jax
import jax.numpy as jnp
from jax import lax
from jax.experimental import pallas as pl
from jax.experimental.pallas import tpu as pltpu
from jax.sharding import Mesh
from jax.sharding import PartitionSpec as P

DOM = ("z", "y", "x_hi", "core")
STAGES = (("z",), ("grp", "y", "x_hi", "core"))
SWAP = ((0, 1), (1, 0))
LANES = 128
SUBSPACES = 64
TILES = 8
HEAD = 8
ROOM = 576
ROWS = HEAD + ROOM + 24
VMEM = pl.BlockSpec(memory_space=pltpu.VMEM)
SMEM = pl.BlockSpec(memory_space=pltpu.SMEM)
ANY = pl.BlockSpec(memory_space=pl.ANY)
HBM = pl.BlockSpec(memory_space=pltpu.HBM)


def positions(levels, i, start):
    l0, l1, l2 = (levels[d, i].astype(jnp.int32) for d in range(3))
    width = l2 + 1
    block = (l1 + 1) * width
    rows = []
    at = start
    for _ in range(4):
        base = jnp.minimum(at, HEAD + ROOM)
        rows += [base, base + width, base + 2 * width, base + 3 * width]
        at = at + block
    return rows, start + (l0 + 1) * block


def owner_tiles(levels, i):
    l0, l1, l2 = (levels[d, i].astype(jnp.int32) for d in range(3))
    row = lax.broadcasted_iota(jnp.int32, (8, LANES), 0)
    fits = (row & 3) <= l2
    return [fits & (k % 2 * 2 + (row >> 2) <= l1) & (k // 2 <= l0) for k in range(TILES)]


def tile_rows(i, k):
    return pl.ds(pl.multiple_of(i * SUBSPACES + k * 8, 8), 8)


def packed_tile(packed_ref, rows, k):
    row = lax.broadcasted_iota(jnp.int32, (8, LANES), 0)
    upper = packed_ref[pl.ds(rows[2 * k], 8), :]
    lower = packed_ref[pl.ds(rows[2 * k + 1] - 4, 8), :]
    return jnp.where(row < 4, upper, lower)


def half_lanes(slot):
    side = lax.axis_index("grp")
    return pl.ds(pl.multiple_of((1 - side if slot else side) * LANES, LANES), LANES)


def cell_tile(surplus_ref, i, k, slot):
    return surplus_ref[i, k * 8 : k * 8 + 8, half_lanes(slot)]


def store_packed(out_ref, rows, k, tile):
    out_ref[pl.ds(rows[2 * k], 4), :] = tile[0:4]
    out_ref[pl.ds(rows[2 * k + 1], 4), :] = tile[4:8]


def pack_far_kernel(levels_ref, surplus_ref, out_ref, held, sems):
    grids = surplus_ref.shape[0]

    def copy(i):
        rows = pl.ds(i * SUBSPACES, SUBSPACES)
        return pltpu.make_async_copy(surplus_ref.at[i, :, half_lanes(1)], held.at[rows, :], sems.at[i])

    for i in range(grids):
        copy(i).start()
    head = jnp.zeros((HEAD, LANES), jnp.float32)
    row = lax.broadcasted_iota(jnp.int32, head.shape, 0)
    lane = lax.broadcasted_iota(jnp.int32, head.shape, 1)
    for d in range(3):
        for i in range(grids):
            head = jnp.where((row == d) & (lane == i), levels_ref[d, i].astype(jnp.float32), head)
    out_ref[0:HEAD, :] = head

    def pack(i, start):
        copy(i).wait()
        rows, stop = positions(levels_ref, i, start)
        for k in range(TILES):
            store_packed(out_ref, rows, k, held[tile_rows(i, k), :])
        return stop

    lax.fori_loop(0, grids, pack, jnp.int32(HEAD))


def pack_far(levels, surplus):
    grids = surplus.shape[0]
    return pl.pallas_call(
        pack_far_kernel,
        out_shape=jax.ShapeDtypeStruct((ROWS, LANES), jnp.float32),
        in_specs=[SMEM, ANY],
        out_specs=VMEM,
        scratch_shapes=[
            pltpu.VMEM((grids * SUBSPACES, LANES), jnp.float32),
            pltpu.SemaphoreType.DMA((grids,)),
        ],
    )(levels, surplus)


def pack_near_kernel(levels_ref, surplus_ref, out_ref):
    grids = surplus_ref.shape[0]
    out_ref[0:HEAD, :] = jnp.zeros((HEAD, LANES), jnp.float32)

    def pack(i, start):
        rows, stop = positions(levels_ref, i, start)
        for k in range(TILES):
            store_packed(out_ref, rows, k, cell_tile(surplus_ref, i, k, 0))
        return stop

    lax.fori_loop(0, grids, pack, jnp.int32(HEAD))


def pack_near(levels, surplus):
    return pl.pallas_call(
        pack_near_kernel,
        out_shape=jax.ShapeDtypeStruct((ROWS, LANES), jnp.float32),
        in_specs=[SMEM, VMEM],
        out_specs=VMEM,
    )(levels, surplus)


def split(ref, s, grids):
    rows = [ref[pl.ds(s + k, grids, stride=SUBSPACES), :] for k in range(8)]
    rows = jnp.concatenate(rows, axis=1)
    high = rows.astype(jnp.bfloat16)
    return high, (rows - high.astype(jnp.float32)).astype(jnp.bfloat16)


def inner(left, right):
    return lax.dot_general(
        jnp.concatenate([left[0], left[0], left[1]], axis=1),
        jnp.concatenate([right[0], right[1], right[0]], axis=1),
        (((1,), (1,)), ((), ())),
        preferred_element_type=jnp.float32,
    )


def own_kernel(levels_ref, surplus_ref, high_ref, low_ref, block_ref, near_ref, far_ref):
    grids = surplus_ref.shape[0]

    def mask(i, carry):
        tiles = owner_tiles(levels_ref, i)
        for k in range(TILES):
            at = tile_rows(i, k)
            near_ref[at, :] = jnp.where(tiles[k], cell_tile(surplus_ref, i, k, 0), 0.0)
            far_ref[at, :] = jnp.where(tiles[k], cell_tile(surplus_ref, i, k, 1), 0.0)
        return carry

    lax.fori_loop(0, grids, mask, 0)
    total = jnp.zeros((grids, grids), jnp.float32)
    for s in range(0, SUBSPACES, 8):
        near = split(near_ref, s, grids)
        far = split(far_ref, s, grids)
        high_ref[:, s * LANES : (s + 8) * LANES] = near[0]
        low_ref[:, s * LANES : (s + 8) * LANES] = near[1]
        total = total + inner(near, near) + inner(far, far)
    block_ref[...] = fold_own(total)


def own_products(levels, surplus):
    grids = surplus.shape[0]
    part = jax.ShapeDtypeStruct((grids, SUBSPACES * LANES), jnp.bfloat16)
    half = pltpu.VMEM((grids * SUBSPACES, LANES), jnp.float32)
    return pl.pallas_call(
        own_kernel,
        out_shape=(part, part, jax.ShapeDtypeStruct((8, LANES), jnp.float32)),
        in_specs=[SMEM, VMEM],
        out_specs=(VMEM, VMEM, VMEM),
        scratch_shapes=[half, half],
    )(levels, surplus)


def fold_own(block):
    strips = [block[r : r + 8, r:] for r in range(0, block.shape[0], 8)]
    used = sum(strip.shape[1] for strip in strips)
    return jnp.concatenate([*strips, jnp.zeros((8, LANES - used), jnp.float32)], axis=1)


def fold_cross(cross):
    grids = cross.shape[0]
    strips = [cross[r : r + 8, :] for r in range(0, grids, 8)]
    ahead = sum(range(8, grids + 8, 8))
    behind = LANES - ahead - grids * len(strips)
    zeros = [jnp.zeros((8, width), jnp.float32) for width in (ahead, behind)]
    return jnp.concatenate([zeros[0], *strips, zeros[1]], axis=1)


def unfold(first, last, grids):
    def strips(folded):
        own, at = [], 0
        for r in range(0, grids, 8):
            strip = folded[:, at : at + grids - r]
            own.append(jnp.concatenate([jnp.zeros((8, r), jnp.float32), strip], axis=1) if r else strip)
            at += grids - r
        cross = [folded[:, at + n * grids : at + (n + 1) * grids] for n in range(grids // 8)]
        return own, cross

    own_first, cross_first = strips(first)
    own_last, cross_last = strips(last)
    half = jnp.concatenate(
        [jnp.concatenate(pair, axis=1) for pair in zip(own_first, cross_first)]
        + [jnp.concatenate(pair, axis=1) for pair in zip(cross_last, own_last)],
        axis=0,
    )
    turned = half.T
    rows = lax.broadcasted_iota(jnp.int32, half.shape, 0)
    columns = lax.broadcasted_iota(jnp.int32, half.shape, 1)
    between = (rows < grids) != (columns < grids)
    gram = jnp.where(rows >> 3 <= columns >> 3, half, turned)
    gram = jnp.where(between, half + turned, gram)
    return jnp.concatenate([gram, jnp.zeros((2 * grids, LANES - 2 * grids), jnp.float32)], axis=1)


def cross_kernel(
    levels_ref, high_ref, low_ref, block_ref, got_ref, parts_ref, full_ref, other_ref, high, low, head, sems
):
    grids = high.shape[0]
    fetch = pltpu.make_async_copy(got_ref.at[0:HEAD, :], head, sems.at[0])
    fetch_high = pltpu.make_async_copy(high_ref, high, sems.at[1])
    fetch_low = pltpu.make_async_copy(low_ref, low, sems.at[2])
    fetch.start()
    fetch_high.start()
    fetch_low.start()
    own = jnp.int32(HEAD)
    for i in range(grids):
        own = own + (levels_ref[0, i] + 1) * (levels_ref[1, i] + 1) * (levels_ref[2, i] + 1)
    fetch.wait()

    def unpack(i, start):
        rows, stop = positions(head, i, start)
        tiles = owner_tiles(head, i)
        for k in range(TILES):
            tile = packed_tile(got_ref, rows, k)
            other_ref[tile_rows(i, k), :] = jnp.where(tiles[k], tile, 0.0)
        return stop

    stop = lax.fori_loop(0, grids, unpack, jnp.int32(HEAD))
    full_ref[0] = (jnp.maximum(own, stop) > HEAD + ROOM).astype(jnp.int32)
    fetch_high.wait()
    fetch_low.wait()
    cross = jnp.zeros((grids, grids), jnp.float32)
    for s in range(0, SUBSPACES, 8):
        at = slice(s * LANES, (s + 8) * LANES)
        cross = cross + inner((high[:, at], low[:, at]), split(other_ref, s, grids))
    folded = block_ref[...] + fold_cross(cross)
    for k in range(parts_ref.shape[0]):
        parts_ref[k] = folded


def cross_products(levels, high, low, block, got, copies):
    grids = high.shape[0]
    return pl.pallas_call(
        cross_kernel,
        out_shape=(
            jax.ShapeDtypeStruct((copies, 8, LANES), jnp.float32),
            jax.ShapeDtypeStruct((1,), jnp.int32),
        ),
        in_specs=[SMEM, HBM, HBM, VMEM, VMEM],
        out_specs=(VMEM, SMEM),
        scratch_shapes=[
            pltpu.VMEM((grids * SUBSPACES, LANES), jnp.float32),
            pltpu.VMEM(high.shape, high.dtype),
            pltpu.VMEM(low.shape, low.dtype),
            pltpu.SMEM((HEAD, LANES), jnp.float32),
            pltpu.SemaphoreType.DMA((3,)),
        ],
    )(levels, high, low, block, got)


def eliminate(parts_ref, grids):
    number = 2 * grids
    senders = parts_ref.shape[0] // 2
    first, last = parts_ref[0], parts_ref[senders]
    for k in range(1, senders):
        first = first + parts_ref[k]
        last = last + parts_ref[senders + k]
    gram = unfold(first, last, grids)
    rows = lax.broadcasted_iota(jnp.int32, gram.shape, 0)
    lanes = lax.broadcasted_iota(jnp.int32, gram.shape, 1)
    on_diagonal = rows == lanes
    diagonal = jnp.sum(jnp.where(on_diagonal, gram, 0.0), axis=1, keepdims=True) + 1e-06
    system = gram + jnp.where(on_diagonal, 0.1 * diagonal, 0.0)
    system = jnp.where(lanes == number, diagonal, system)
    for first in range(0, number, 8):
        columns = [
            jnp.broadcast_to(system[:, k : k + 1], system.shape) for k in range(first, first + 8)
        ]
        for j in range(8):
            k = first + j
            inverse = 1.0 / columns[j][k : k + 1, :]
            column = jnp.where(rows == k, 0.0, columns[j])
            system = system - column * (system[k : k + 1, :] * inverse)
            for q in range(j + 1, 8):
                scale = columns[j][first + q : first + q + 1, :] * inverse
                columns[q] = columns[q] - column * scale
    last = jnp.broadcast_to(system[:, number : number + 1], system.shape)
    solved = jnp.where(on_diagonal, last / system, 0.0)
    return jnp.broadcast_to(jnp.sum(solved, axis=1, keepdims=True), system.shape), on_diagonal


def solve_kernel(parts_ref, out_ref):
    solution_rows, on_diagonal = eliminate(parts_ref, out_ref.shape[1] // 2)
    out_ref[...] = jnp.sum(jnp.where(on_diagonal, solution_rows, 0.0), axis=0, keepdims=True)[:, : out_ref.shape[1]]


def solve_parts(parts, grids):
    return pl.pallas_call(
        solve_kernel,
        out_shape=jax.ShapeDtypeStruct((1, 2 * grids), jnp.float32),
        in_specs=[VMEM],
        out_specs=VMEM,
    )(parts)


def finish_kernel(
    levels_ref,
    parts_ref,
    surplus_ref,
    got_near_ref,
    got_far_ref,
    updated_ref,
    out_ref,
    head,
    head_sem,
    weights,
    line,
    line_sem,
    result,
    out_sems,
):
    grids = surplus_ref.shape[0]
    side = lax.axis_index("grp")
    fetch = pltpu.make_async_copy(got_near_ref.at[0:HEAD, :], head, head_sem)
    fetch.start()
    solution_rows, on_diagonal = eliminate(parts_ref, grids)
    weights[...] = solution_rows
    line[...] = jnp.sum(jnp.where(on_diagonal, solution_rows, 0.0), axis=0, keepdims=True)[:, : line.shape[1]]
    send_line = pltpu.make_async_copy(line, out_ref, line_sem)
    send_line.start()
    fetch.wait()

    def add(i, carry):
        start, sums = carry
        rows, stop = positions(head, i, start)
        own_tiles = owner_tiles(levels_ref, i)
        other_tiles = owner_tiles(head, i)
        own = jnp.broadcast_to(weights[pl.ds(side * grids + i, 1), :], (8, LANES))
        other = jnp.broadcast_to(weights[pl.ds((1 - side) * grids + i, 1), :], (8, LANES))
        added = []
        for slot, got in ((0, got_near_ref), (1, got_far_ref)):
            for k in range(TILES):
                mine = jnp.where(own_tiles[k], cell_tile(surplus_ref, i, k, slot), 0.0)
                theirs = jnp.where(other_tiles[k], packed_tile(got, rows, k), 0.0)
                added.append(sums[slot * TILES + k] + own * mine + other * theirs)
        return stop, tuple(added)

    zero = jnp.zeros((8, LANES), jnp.float32)
    _, sums = lax.fori_loop(0, grids, add, (jnp.int32(HEAD), (zero,) * (2 * TILES)))

    def put(i, slot):
        rows = pl.ds(i * SUBSPACES, SUBSPACES)
        return pltpu.make_async_copy(result.at[slot, rows, :], updated_ref.at[i, :, half_lanes(slot)], out_sems.at[slot, i])

    def spread(i, carry):
        tiles = owner_tiles(levels_ref, i)
        for slot in range(2):
            for k in range(TILES):
                result[slot, tile_rows(i, k), :] = jnp.where(tiles[k], sums[slot * TILES + k], 0.0)
            put(i, slot).start()
        return carry

    lax.fori_loop(0, grids, spread, 0)
    send_line.wait()
    for i in range(grids):
        put(i, 0).wait()
        put(i, 1).wait()


def finish(levels, parts, surplus, got_near, got_far):
    grids = surplus.shape[0]
    return pl.pallas_call(
        finish_kernel,
        out_shape=(
            jax.ShapeDtypeStruct(surplus.shape, jnp.float32),
            jax.ShapeDtypeStruct((1, 2 * grids), jnp.float32),
        ),
        in_specs=[SMEM, VMEM, VMEM, VMEM, VMEM],
        out_specs=(HBM, HBM),
        scratch_shapes=[
            pltpu.SMEM((HEAD, LANES), jnp.float32),
            pltpu.SemaphoreType.DMA,
            pltpu.VMEM((2 * grids, LANES), jnp.float32),
            pltpu.VMEM((1, 2 * grids), jnp.float32),
            pltpu.SemaphoreType.DMA,
            pltpu.VMEM((2, grids * SUBSPACES, LANES), jnp.float32),
            pltpu.SemaphoreType.DMA((2, grids)),
        ],
    )(levels, parts, surplus, got_near, got_far)


def owned(levels, count):
    indices = jnp.arange(count, dtype=jnp.int32)
    digits = jnp.stack([indices // 16, indices // 4 % 4, indices % 4])
    return jnp.all(digits[:, None] <= levels[:, :, None], axis=0).astype(jnp.float32)


def halves(levels, surplus):
    second = lax.axis_index("grp") == 1
    masked = surplus * owned(levels, SUBSPACES)[:, :, None]
    low, high = masked[:, :, :LANES], masked[:, :, LANES:]
    return jnp.where(second, high, low), jnp.where(second, low, high)


def dense_finish(levels, surplus):
    grids = surplus.shape[0]
    second = lax.axis_index("grp") == 1
    near, far = halves(levels, surplus)
    got_near = lax.ppermute(far, "grp", SWAP)
    got_far = lax.ppermute(near, "grp", SWAP)

    def products(left, right):
        return lax.dot_general(
            left,
            right,
            (((1, 2), (1, 2)), ((), ())),
            precision=lax.Precision.HIGHEST,
            preferred_element_type=jnp.float32,
        )

    cross = products(near, got_near)
    own = products(near, near) + products(far, far)
    folded = fold_own(own) + fold_cross(cross)
    pair = jnp.stack([jnp.where(second, 0.0, folded), jnp.where(second, folded, 0.0)])
    for axis in ("grp", *DOM):
        pair = lax.psum(pair, axis)
    coefficients = solve_parts(pair, grids)
    start, stop = coefficients[0, :grids], coefficients[0, grids:]
    own = jnp.where(second, stop, start)[:, None, None]
    other = jnp.where(second, start, stop)[:, None, None]
    sum_near = jnp.sum(own * near + other * got_near, axis=0)
    sum_far = jnp.sum(own * far + other * got_far, axis=0)
    combined = jnp.concatenate(
        [jnp.where(second, sum_far, sum_near), jnp.where(second, sum_near, sum_far)], axis=1
    )
    return owned(levels, SUBSPACES)[:, :, None] * combined[None], coefficients


def exchanged(copies, axes):
    return lax.all_to_all(copies, axes, split_axis=0, concat_axis=0, tiled=True)


def whole(surplus, levels):
    levels = levels.T
    far = pack_far(levels, surplus)
    got_near = lax.ppermute(far, "grp", SWAP)
    near = pack_near(levels, surplus)
    got_far = lax.ppermute(near, "grp", SWAP)
    high, low, block = own_products(levels, surplus)
    parts, full = cross_products(levels, high, low, block, got_near, lax.axis_size(STAGES[0]))
    for axes, following in zip(STAGES, STAGES[1:]):
        folded = jnp.sum(exchanged(parts, axes), axis=0)
        parts = jnp.broadcast_to(folded, (lax.axis_size(following), *folded.shape))
    parts = exchanged(parts, STAGES[-1])
    updated, coefficients = lax.cond(
        full[0] > 0,
        lambda: dense_finish(levels, surplus),
        lambda: tuple(finish(levels, parts, surplus, got_near, got_far)),
    )
    return updated, coefficients.reshape(-1)


def solution(mesh):
    torus = Mesh(
        mesh.devices.reshape(mesh.shape["grp"], 8, 8, 2, 2),
        ("grp", *DOM),
    )
    return jax.shard_map(
        whole,
        mesh=torus,
        in_specs=(P("grp", None, DOM), P("grp", None)),
        out_specs=(P("grp", None, DOM), P()),
        check_vma=False,
    )
```

```python
import jax
import jax.numpy as jnp
from jax import lax
from jax.experimental import pallas as pl
from jax.experimental.pallas import tpu as pltpu
from jax.sharding import Mesh
from jax.sharding import PartitionSpec as P

DOM = ("z", "y", "x_hi", "core")
STAGES = (("z",), ("grp", "y", "x_hi", "core"))
SWAP = ((0, 1), (1, 0))
LANES = 128
SUBSPACES = 64
TILES = 8
HEAD = 8
ROOM = 576
ROWS = HEAD + ROOM + 24
VMEM = pl.BlockSpec(memory_space=pltpu.VMEM)
SMEM = pl.BlockSpec(memory_space=pltpu.SMEM)
ANY = pl.BlockSpec(memory_space=pl.ANY)
GRANT = pltpu.CompilerParams(vmem_limit_bytes=12 << 20)


def positions(levels, i, start):
    l0, l1, l2 = (levels[d, i].astype(jnp.int32) for d in range(3))
    width = l2 + 1
    block = (l1 + 1) * width
    rows = []
    at = start
    for _ in range(4):
        base = jnp.minimum(at, HEAD + ROOM)
        rows += [base, base + width, base + 2 * width, base + 3 * width]
        at = at + block
    return rows, start + (l0 + 1) * block


def owner_tiles(levels, i):
    l0, l1, l2 = (levels[d, i].astype(jnp.int32) for d in range(3))
    row = lax.broadcasted_iota(jnp.int32, (8, LANES), 0)
    fits = (row & 3) <= l2
    return [fits & (k % 2 * 2 + (row >> 2) <= l1) & (k // 2 <= l0) for k in range(TILES)]


def tile_rows(i, k):
    return pl.ds(pl.multiple_of(i * SUBSPACES + k * 8, 8), 8)


def packed_tile(packed_ref, rows, k):
    row = lax.broadcasted_iota(jnp.int32, (8, LANES), 0)
    upper = packed_ref[pl.ds(rows[2 * k], 8), :]
    lower = packed_ref[pl.ds(rows[2 * k + 1] - 4, 8), :]
    return jnp.where(row < 4, upper, lower)


def half_lanes(slot):
    side = lax.axis_index("grp")
    return pl.ds(pl.multiple_of((1 - side if slot else side) * LANES, LANES), LANES)


def cell_tile(surplus_ref, i, k, slot):
    return surplus_ref[i, k * 8 : k * 8 + 8, half_lanes(slot)]


def store_packed(out_ref, rows, k, tile):
    out_ref[pl.ds(rows[2 * k], 4), :] = tile[0:4]
    out_ref[pl.ds(rows[2 * k + 1], 4), :] = tile[4:8]


def pack_far_kernel(levels_ref, surplus_ref, out_ref, held, sems):
    grids = surplus_ref.shape[0]

    def copy(i):
        rows = pl.ds(i * SUBSPACES, SUBSPACES)
        return pltpu.make_async_copy(surplus_ref.at[i, :, half_lanes(1)], held.at[rows, :], sems.at[i])

    for i in range(grids):
        copy(i).start()
    head = jnp.zeros((HEAD, LANES), jnp.float32)
    row = lax.broadcasted_iota(jnp.int32, head.shape, 0)
    lane = lax.broadcasted_iota(jnp.int32, head.shape, 1)
    for d in range(3):
        for i in range(grids):
            head = jnp.where((row == d) & (lane == i), levels_ref[d, i].astype(jnp.float32), head)
    out_ref[0:HEAD, :] = head

    def pack(i, start):
        copy(i).wait()
        rows, stop = positions(levels_ref, i, start)
        for k in range(TILES):
            store_packed(out_ref, rows, k, held[tile_rows(i, k), :])
        return stop

    lax.fori_loop(0, grids, pack, jnp.int32(HEAD))


def pack_far(levels, surplus):
    grids = surplus.shape[0]
    return pl.pallas_call(
        pack_far_kernel,
        compiler_params=GRANT,
        out_shape=jax.ShapeDtypeStruct((ROWS, LANES), jnp.float32),
        in_specs=[SMEM, ANY],
        out_specs=VMEM,
        scratch_shapes=[
            pltpu.VMEM((grids * SUBSPACES, LANES), jnp.float32),
            pltpu.SemaphoreType.DMA((grids,)),
        ],
    )(levels, surplus)


def pack_near_kernel(levels_ref, surplus_ref, out_ref):
    grids = surplus_ref.shape[0]
    out_ref[0:HEAD, :] = jnp.zeros((HEAD, LANES), jnp.float32)

    def pack(i, start):
        rows, stop = positions(levels_ref, i, start)
        for k in range(TILES):
            store_packed(out_ref, rows, k, cell_tile(surplus_ref, i, k, 0))
        return stop

    lax.fori_loop(0, grids, pack, jnp.int32(HEAD))


def pack_near(levels, surplus):
    return pl.pallas_call(
        pack_near_kernel,
        compiler_params=GRANT,
        out_shape=jax.ShapeDtypeStruct((ROWS, LANES), jnp.float32),
        in_specs=[SMEM, VMEM],
        out_specs=VMEM,
    )(levels, surplus)


def split(ref, s, grids):
    rows = [ref[pl.ds(s + k, grids, stride=SUBSPACES), :] for k in range(8)]
    rows = jnp.concatenate(rows, axis=1)
    high = rows.astype(jnp.bfloat16)
    return high, (rows - high.astype(jnp.float32)).astype(jnp.bfloat16)


def inner(left, right):
    return lax.dot_general(
        jnp.concatenate([left[0], left[0], left[1]], axis=1),
        jnp.concatenate([right[0], right[1], right[0]], axis=1),
        (((1,), (1,)), ((), ())),
        preferred_element_type=jnp.float32,
    )


def own_kernel(levels_ref, surplus_ref, high_ref, low_ref, block_ref, near_ref, far_ref):
    grids = surplus_ref.shape[0]

    def mask(i, carry):
        tiles = owner_tiles(levels_ref, i)
        for k in range(TILES):
            at = tile_rows(i, k)
            near_ref[at, :] = jnp.where(tiles[k], cell_tile(surplus_ref, i, k, 0), 0.0)
            far_ref[at, :] = jnp.where(tiles[k], cell_tile(surplus_ref, i, k, 1), 0.0)
        return carry

    lax.fori_loop(0, grids, mask, 0)
    total = jnp.zeros((grids, grids), jnp.float32)
    for s in range(0, SUBSPACES, 8):
        near = split(near_ref, s, grids)
        far = split(far_ref, s, grids)
        high_ref[:, s * LANES : (s + 8) * LANES] = near[0]
        low_ref[:, s * LANES : (s + 8) * LANES] = near[1]
        total = total + inner(near, near) + inner(far, far)
    block_ref[...] = fold_own(total)


def own_products(levels, surplus):
    grids = surplus.shape[0]
    part = jax.ShapeDtypeStruct((grids, SUBSPACES * LANES), jnp.bfloat16)
    half = pltpu.VMEM((grids * SUBSPACES, LANES), jnp.float32)
    return pl.pallas_call(
        own_kernel,
        compiler_params=GRANT,
        out_shape=(part, part, jax.ShapeDtypeStruct((8, LANES), jnp.float32)),
        in_specs=[SMEM, VMEM],
        out_specs=(VMEM, VMEM, VMEM),
        scratch_shapes=[half, half],
    )(levels, surplus)


def fold_own(block):
    strips = [block[r : r + 8, r:] for r in range(0, block.shape[0], 8)]
    used = sum(strip.shape[1] for strip in strips)
    return jnp.concatenate([*strips, jnp.zeros((8, LANES - used), jnp.float32)], axis=1)


def fold_cross(cross):
    grids = cross.shape[0]
    strips = [cross[r : r + 8, :] for r in range(0, grids, 8)]
    ahead = sum(range(8, grids + 8, 8))
    behind = LANES - ahead - grids * len(strips)
    zeros = [jnp.zeros((8, width), jnp.float32) for width in (ahead, behind)]
    return jnp.concatenate([zeros[0], *strips, zeros[1]], axis=1)


def unfold(first, last, grids):
    def strips(folded):
        own, at = [], 0
        for r in range(0, grids, 8):
            strip = folded[:, at : at + grids - r]
            own.append(jnp.concatenate([jnp.zeros((8, r), jnp.float32), strip], axis=1) if r else strip)
            at += grids - r
        cross = [folded[:, at + n * grids : at + (n + 1) * grids] for n in range(grids // 8)]
        return own, cross

    own_first, cross_first = strips(first)
    own_last, cross_last = strips(last)
    half = jnp.concatenate(
        [jnp.concatenate(pair, axis=1) for pair in zip(own_first, cross_first)]
        + [jnp.concatenate(pair, axis=1) for pair in zip(cross_last, own_last)],
        axis=0,
    )
    turned = half.T
    rows = lax.broadcasted_iota(jnp.int32, half.shape, 0)
    columns = lax.broadcasted_iota(jnp.int32, half.shape, 1)
    between = (rows < grids) != (columns < grids)
    gram = jnp.where(rows >> 3 <= columns >> 3, half, turned)
    gram = jnp.where(between, half + turned, gram)
    return jnp.concatenate([gram, jnp.zeros((2 * grids, LANES - 2 * grids), jnp.float32)], axis=1)


def cross_kernel(
    levels_ref, high_ref, low_ref, block_ref, got_ref, parts_ref, full_ref, other_ref, head, sem
):
    grids = high_ref.shape[0]
    fetch = pltpu.make_async_copy(got_ref.at[0:HEAD, :], head, sem)
    fetch.start()
    own = jnp.int32(HEAD)
    for i in range(grids):
        own = own + (levels_ref[0, i] + 1) * (levels_ref[1, i] + 1) * (levels_ref[2, i] + 1)
    fetch.wait()

    def unpack(i, start):
        rows, stop = positions(head, i, start)
        tiles = owner_tiles(head, i)
        for k in range(TILES):
            tile = packed_tile(got_ref, rows, k)
            other_ref[tile_rows(i, k), :] = jnp.where(tiles[k], tile, 0.0)
        return stop

    stop = lax.fori_loop(0, grids, unpack, jnp.int32(HEAD))
    full_ref[0] = (jnp.maximum(own, stop) > HEAD + ROOM).astype(jnp.int32)
    cross = jnp.zeros((grids, grids), jnp.float32)
    for s in range(0, SUBSPACES, 8):
        at = slice(s * LANES, (s + 8) * LANES)
        cross = cross + inner((high_ref[:, at], low_ref[:, at]), split(other_ref, s, grids))
    folded = block_ref[...] + fold_cross(cross)
    for k in range(parts_ref.shape[0]):
        parts_ref[k] = folded


def cross_products(levels, high, low, block, got, copies):
    grids = high.shape[0]
    return pl.pallas_call(
        cross_kernel,
        compiler_params=GRANT,
        out_shape=(
            jax.ShapeDtypeStruct((copies, 8, LANES), jnp.float32),
            jax.ShapeDtypeStruct((1,), jnp.int32),
        ),
        in_specs=[SMEM, VMEM, VMEM, VMEM, VMEM],
        out_specs=(VMEM, SMEM),
        scratch_shapes=[
            pltpu.VMEM((grids * SUBSPACES, LANES), jnp.float32),
            pltpu.SMEM((HEAD, LANES), jnp.float32),
            pltpu.SemaphoreType.DMA,
        ],
    )(levels, high, low, block, got)


def eliminate(parts_ref, grids):
    number = 2 * grids
    senders = parts_ref.shape[0] // 2
    first, last = parts_ref[0], parts_ref[senders]
    for k in range(1, senders):
        first = first + parts_ref[k]
        last = last + parts_ref[senders + k]
    gram = unfold(first, last, grids)
    rows = lax.broadcasted_iota(jnp.int32, gram.shape, 0)
    lanes = lax.broadcasted_iota(jnp.int32, gram.shape, 1)
    on_diagonal = rows == lanes
    diagonal = jnp.sum(jnp.where(on_diagonal, gram, 0.0), axis=1, keepdims=True) + 1e-06
    system = gram + jnp.where(on_diagonal, 0.1 * diagonal, 0.0)
    system = jnp.where(lanes == number, diagonal, system)
    for first in range(0, number, 8):
        columns = [
            jnp.broadcast_to(system[:, k : k + 1], system.shape) for k in range(first, first + 8)
        ]
        for j in range(8):
            k = first + j
            inverse = 1.0 / columns[j][k : k + 1, :]
            column = jnp.where(rows == k, 0.0, columns[j])
            system = system - column * (system[k : k + 1, :] * inverse)
            for q in range(j + 1, 8):
                scale = columns[j][first + q : first + q + 1, :] * inverse
                columns[q] = columns[q] - column * scale
    last = jnp.broadcast_to(system[:, number : number + 1], system.shape)
    solved = jnp.where(on_diagonal, last / system, 0.0)
    return jnp.broadcast_to(jnp.sum(solved, axis=1, keepdims=True), system.shape), on_diagonal


def solve_kernel(parts_ref, out_ref):
    solution_rows, on_diagonal = eliminate(parts_ref, out_ref.shape[1] // 2)
    out_ref[...] = jnp.sum(jnp.where(on_diagonal, solution_rows, 0.0), axis=0, keepdims=True)[:, : out_ref.shape[1]]


def solve_parts(parts, grids):
    return pl.pallas_call(
        solve_kernel,
        compiler_params=GRANT,
        out_shape=jax.ShapeDtypeStruct((1, 2 * grids), jnp.float32),
        in_specs=[VMEM],
        out_specs=VMEM,
    )(parts)


def finish_kernel(
    levels_ref,
    parts_ref,
    surplus_ref,
    got_near_ref,
    got_far_ref,
    updated_ref,
    out_ref,
    head,
    head_sem,
    weights,
    result,
    out_sems,
):
    grids = surplus_ref.shape[0]
    side = lax.axis_index("grp")
    fetch = pltpu.make_async_copy(got_near_ref.at[0:HEAD, :], head, head_sem)
    fetch.start()
    solution_rows, on_diagonal = eliminate(parts_ref, grids)
    weights[...] = solution_rows
    out_ref[...] = jnp.sum(jnp.where(on_diagonal, solution_rows, 0.0), axis=0, keepdims=True)[:, : out_ref.shape[1]]
    fetch.wait()

    def add(i, carry):
        start, sums = carry
        rows, stop = positions(head, i, start)
        own_tiles = owner_tiles(levels_ref, i)
        other_tiles = owner_tiles(head, i)
        own = jnp.broadcast_to(weights[pl.ds(side * grids + i, 1), :], (8, LANES))
        other = jnp.broadcast_to(weights[pl.ds((1 - side) * grids + i, 1), :], (8, LANES))
        added = []
        for slot, got in ((0, got_near_ref), (1, got_far_ref)):
            for k in range(TILES):
                mine = jnp.where(own_tiles[k], cell_tile(surplus_ref, i, k, slot), 0.0)
                theirs = jnp.where(other_tiles[k], packed_tile(got, rows, k), 0.0)
                added.append(sums[slot * TILES + k] + own * mine + other * theirs)
        return stop, tuple(added)

    zero = jnp.zeros((8, LANES), jnp.float32)
    _, sums = lax.fori_loop(0, grids, add, (jnp.int32(HEAD), (zero,) * (2 * TILES)))

    def put(i, slot):
        rows = pl.ds(i * SUBSPACES, SUBSPACES)
        return pltpu.make_async_copy(result.at[slot, rows, :], updated_ref.at[i, :, half_lanes(slot)], out_sems.at[slot, i])

    def spread(i, carry):
        tiles = owner_tiles(levels_ref, i)
        for slot in range(2):
            for k in range(TILES):
                result[slot, tile_rows(i, k), :] = jnp.where(tiles[k], sums[slot * TILES + k], 0.0)
            put(i, slot).start()
        return carry

    lax.fori_loop(0, grids, spread, 0)
    for i in range(grids):
        put(i, 0).wait()
        put(i, 1).wait()


def finish(levels, parts, surplus, got_near, got_far):
    grids = surplus.shape[0]
    return pl.pallas_call(
        finish_kernel,
        compiler_params=GRANT,
        out_shape=(
            jax.ShapeDtypeStruct(surplus.shape, jnp.float32),
            jax.ShapeDtypeStruct((1, 2 * grids), jnp.float32),
        ),
        in_specs=[SMEM, VMEM, VMEM, VMEM, VMEM],
        out_specs=(ANY, VMEM),
        scratch_shapes=[
            pltpu.SMEM((HEAD, LANES), jnp.float32),
            pltpu.SemaphoreType.DMA,
            pltpu.VMEM((2 * grids, LANES), jnp.float32),
            pltpu.VMEM((2, grids * SUBSPACES, LANES), jnp.float32),
            pltpu.SemaphoreType.DMA((2, grids)),
        ],
    )(levels, parts, surplus, got_near, got_far)


def owned(levels, count):
    indices = jnp.arange(count, dtype=jnp.int32)
    digits = jnp.stack([indices // 16, indices // 4 % 4, indices % 4])
    return jnp.all(digits[:, None] <= levels[:, :, None], axis=0).astype(jnp.float32)


def halves(levels, surplus):
    second = lax.axis_index("grp") == 1
    masked = surplus * owned(levels, SUBSPACES)[:, :, None]
    low, high = masked[:, :, :LANES], masked[:, :, LANES:]
    return jnp.where(second, high, low), jnp.where(second, low, high)


def dense_finish(levels, surplus):
    grids = surplus.shape[0]
    second = lax.axis_index("grp") == 1
    near, far = halves(levels, surplus)
    got_near = lax.ppermute(far, "grp", SWAP)
    got_far = lax.ppermute(near, "grp", SWAP)

    def products(left, right):
        return lax.dot_general(
            left,
            right,
            (((1, 2), (1, 2)), ((), ())),
            precision=lax.Precision.HIGHEST,
            preferred_element_type=jnp.float32,
        )

    cross = products(near, got_near)
    own = products(near, near) + products(far, far)
    folded = fold_own(own) + fold_cross(cross)
    pair = jnp.stack([jnp.where(second, 0.0, folded), jnp.where(second, folded, 0.0)])
    for axis in ("grp", *DOM):
        pair = lax.psum(pair, axis)
    coefficients = solve_parts(pair, grids)
    start, stop = coefficients[0, :grids], coefficients[0, grids:]
    own = jnp.where(second, stop, start)[:, None, None]
    other = jnp.where(second, start, stop)[:, None, None]
    sum_near = jnp.sum(own * near + other * got_near, axis=0)
    sum_far = jnp.sum(own * far + other * got_far, axis=0)
    combined = jnp.concatenate(
        [jnp.where(second, sum_far, sum_near), jnp.where(second, sum_near, sum_far)], axis=1
    )
    return owned(levels, SUBSPACES)[:, :, None] * combined[None], coefficients


def exchanged(copies, axes):
    return lax.all_to_all(copies, axes, split_axis=0, concat_axis=0, tiled=True)


def whole(surplus, levels):
    levels = levels.T
    far = pack_far(levels, surplus)
    got_near = lax.ppermute(far, "grp", SWAP)
    near = pack_near(levels, surplus)
    got_far = lax.ppermute(near, "grp", SWAP)
    high, low, block = own_products(levels, surplus)
    parts, full = cross_products(levels, high, low, block, got_near, lax.axis_size(STAGES[0]))
    for axes, following in zip(STAGES, STAGES[1:]):
        folded = jnp.sum(exchanged(parts, axes), axis=0)
        parts = jnp.broadcast_to(folded, (lax.axis_size(following), *folded.shape))
    parts = exchanged(parts, STAGES[-1])
    updated, coefficients = lax.cond(
        full[0] > 0,
        lambda: dense_finish(levels, surplus),
        lambda: tuple(finish(levels, parts, surplus, got_near, got_far)),
    )
    return updated, coefficients.reshape(-1)


def solution(mesh):
    torus = Mesh(
        mesh.devices.reshape(mesh.shape["grp"], 8, 8, 2, 2),
        ("grp", *DOM),
    )
    return jax.shard_map(
        whole,
        mesh=torus,
        in_specs=(P("grp", None, DOM), P("grp", None)),
        out_specs=(P("grp", None, DOM), P()),
        check_vma=False,
    )
```

```python
import jax
import jax.numpy as jnp
from jax import lax
from jax.experimental import pallas as pl
from jax.experimental.pallas import tpu as pltpu
from jax.sharding import Mesh
from jax.sharding import PartitionSpec as P

DOM = ("z", "y", "x_hi", "core")
STAGES = (("z",), ("grp", "y", "x_hi", "core"))
SWAP = ((0, 1), (1, 0))
LANES = 128
SUBSPACES = 64
TILES = 8
HEAD = 8
ROOM = 576
ROWS = HEAD + ROOM + 24
VMEM = pl.BlockSpec(memory_space=pltpu.VMEM)
SMEM = pl.BlockSpec(memory_space=pltpu.SMEM)
ANY = pl.BlockSpec(memory_space=pl.ANY)
GRANT = pltpu.CompilerParams(vmem_limit_bytes=12 << 20)


def positions(levels, i, start):
    l0, l1, l2 = (levels[d, i].astype(jnp.int32) for d in range(3))
    width = l2 + 1
    block = (l1 + 1) * width
    rows = []
    at = start
    for _ in range(4):
        base = jnp.minimum(at, HEAD + ROOM)
        rows += [base, base + width, base + 2 * width, base + 3 * width]
        at = at + block
    return rows, start + (l0 + 1) * block


def owner_tiles(levels, i):
    l0, l1, l2 = (levels[d, i].astype(jnp.int32) for d in range(3))
    row = lax.broadcasted_iota(jnp.int32, (8, LANES), 0)
    fits = (row & 3) <= l2
    return [fits & (k % 2 * 2 + (row >> 2) <= l1) & (k // 2 <= l0) for k in range(TILES)]


def tile_rows(i, k):
    return pl.ds(pl.multiple_of(i * SUBSPACES + k * 8, 8), 8)


def packed_tile(packed_ref, rows, k):
    row = lax.broadcasted_iota(jnp.int32, (8, LANES), 0)
    upper = packed_ref[pl.ds(rows[2 * k], 8), :]
    lower = packed_ref[pl.ds(rows[2 * k + 1] - 4, 8), :]
    return jnp.where(row < 4, upper, lower)


def half_lanes(slot):
    side = lax.axis_index("grp")
    return pl.ds(pl.multiple_of((1 - side if slot else side) * LANES, LANES), LANES)


def cell_tile(surplus_ref, i, k, slot):
    return surplus_ref[i, k * 8 : k * 8 + 8, half_lanes(slot)]


def store_packed(out_ref, rows, k, tile):
    out_ref[pl.ds(rows[2 * k], 4), :] = tile[0:4]
    out_ref[pl.ds(rows[2 * k + 1], 4), :] = tile[4:8]


def pack_far_kernel(levels_ref, surplus_ref, out_ref, held, sems):
    grids = surplus_ref.shape[0]

    def copy(i):
        rows = pl.ds(i * SUBSPACES, SUBSPACES)
        return pltpu.make_async_copy(surplus_ref.at[i, :, half_lanes(1)], held.at[rows, :], sems.at[i])

    for i in range(grids):
        copy(i).start()
    head = jnp.zeros((HEAD, LANES), jnp.float32)
    row = lax.broadcasted_iota(jnp.int32, head.shape, 0)
    lane = lax.broadcasted_iota(jnp.int32, head.shape, 1)
    for d in range(3):
        for i in range(grids):
            head = jnp.where((row == d) & (lane == i), levels_ref[d, i].astype(jnp.float32), head)
    out_ref[0:HEAD, :] = head

    def pack(i, start):
        copy(i).wait()
        rows, stop = positions(levels_ref, i, start)
        for k in range(TILES):
            store_packed(out_ref, rows, k, held[tile_rows(i, k), :])
        return stop

    over_grids(grids, pack, jnp.int32(HEAD))


def pack_far(levels, surplus):
    grids = surplus.shape[0]
    return pl.pallas_call(
        pack_far_kernel,
        compiler_params=GRANT,
        out_shape=jax.ShapeDtypeStruct((ROWS, LANES), jnp.float32),
        in_specs=[SMEM, ANY],
        out_specs=VMEM,
        scratch_shapes=[
            pltpu.VMEM((grids * SUBSPACES, LANES), jnp.float32),
            pltpu.SemaphoreType.DMA((grids,)),
        ],
    )(levels, surplus)


def pack_near_kernel(levels_ref, surplus_ref, out_ref):
    grids = surplus_ref.shape[0]
    out_ref[0:HEAD, :] = jnp.zeros((HEAD, LANES), jnp.float32)

    def pack(i, start):
        rows, stop = positions(levels_ref, i, start)
        for k in range(TILES):
            store_packed(out_ref, rows, k, cell_tile(surplus_ref, i, k, 0))
        return stop

    over_grids(grids, pack, jnp.int32(HEAD))


def pack_near(levels, surplus):
    return pl.pallas_call(
        pack_near_kernel,
        compiler_params=GRANT,
        out_shape=jax.ShapeDtypeStruct((ROWS, LANES), jnp.float32),
        in_specs=[SMEM, VMEM],
        out_specs=VMEM,
    )(levels, surplus)


def over_grids(grids, body, init):
    def step(n, carry):
        return body(2 * n + 1, body(2 * n, carry))

    return lax.fori_loop(0, grids // 2, step, init)


def split(ref, s, grids):
    rows = [ref[pl.ds(s + k, grids, stride=SUBSPACES), :] for k in range(8)]
    rows = jnp.concatenate(rows, axis=1)
    high = rows.astype(jnp.bfloat16).astype(jnp.float32)
    return jnp.concatenate([high, rows - high], axis=0).astype(jnp.bfloat16)


def inner(left, right):
    return lax.dot_general(
        left, right, (((1,), (1,)), ((), ())), preferred_element_type=jnp.float32
    )


def whole_products(total):
    grids = total.shape[0] // 2
    rows = total[:grids, :] + total[grids:, :]
    return rows[:, :grids] + rows[:, grids:]


def own_kernel(levels_ref, surplus_ref, both_ref, block_ref, near_ref, far_ref):
    grids = surplus_ref.shape[0]

    def mask(i, carry):
        tiles = owner_tiles(levels_ref, i)
        for k in range(TILES):
            at = tile_rows(i, k)
            near_ref[at, :] = jnp.where(tiles[k], cell_tile(surplus_ref, i, k, 0), 0.0)
            far_ref[at, :] = jnp.where(tiles[k], cell_tile(surplus_ref, i, k, 1), 0.0)
        return carry

    over_grids(grids, mask, 0)
    total = jnp.zeros((2 * grids, 2 * grids), jnp.float32)
    for s in range(0, SUBSPACES, 8):
        near = split(near_ref, s, grids)
        far = split(far_ref, s, grids)
        both_ref[:, s * LANES : (s + 8) * LANES] = near
        total = total + inner(near, near) + inner(far, far)
    block_ref[...] = fold_own(whole_products(total))


def own_products(levels, surplus):
    grids = surplus.shape[0]
    both = jax.ShapeDtypeStruct((2 * grids, SUBSPACES * LANES), jnp.bfloat16)
    half = pltpu.VMEM((grids * SUBSPACES, LANES), jnp.float32)
    return pl.pallas_call(
        own_kernel,
        compiler_params=GRANT,
        out_shape=(both, jax.ShapeDtypeStruct((8, LANES), jnp.float32)),
        in_specs=[SMEM, VMEM],
        out_specs=(VMEM, VMEM),
        scratch_shapes=[half, half],
    )(levels, surplus)


def fold_own(block):
    strips = [block[r : r + 8, r:] for r in range(0, block.shape[0], 8)]
    used = sum(strip.shape[1] for strip in strips)
    return jnp.concatenate([*strips, jnp.zeros((8, LANES - used), jnp.float32)], axis=1)


def fold_cross(cross):
    grids = cross.shape[0]
    strips = [cross[r : r + 8, :] for r in range(0, grids, 8)]
    ahead = sum(range(8, grids + 8, 8))
    behind = LANES - ahead - grids * len(strips)
    zeros = [jnp.zeros((8, width), jnp.float32) for width in (ahead, behind)]
    return jnp.concatenate([zeros[0], *strips, zeros[1]], axis=1)


def unfold(first, last, grids):
    def strips(folded):
        own, at = [], 0
        for r in range(0, grids, 8):
            strip = folded[:, at : at + grids - r]
            own.append(jnp.concatenate([jnp.zeros((8, r), jnp.float32), strip], axis=1) if r else strip)
            at += grids - r
        cross = [folded[:, at + n * grids : at + (n + 1) * grids] for n in range(grids // 8)]
        return own, cross

    own_first, cross_first = strips(first)
    own_last, cross_last = strips(last)
    half = jnp.concatenate(
        [jnp.concatenate(pair, axis=1) for pair in zip(own_first, cross_first)]
        + [jnp.concatenate(pair, axis=1) for pair in zip(cross_last, own_last)],
        axis=0,
    )
    turned = half.T
    rows = lax.broadcasted_iota(jnp.int32, half.shape, 0)
    columns = lax.broadcasted_iota(jnp.int32, half.shape, 1)
    between = (rows < grids) != (columns < grids)
    gram = jnp.where(rows >> 3 <= columns >> 3, half, turned)
    gram = jnp.where(between, half + turned, gram)
    return jnp.concatenate([gram, jnp.zeros((2 * grids, LANES - 2 * grids), jnp.float32)], axis=1)


def cross_kernel(
    levels_ref, both_ref, block_ref, got_ref, parts_ref, full_ref, other_ref, head, sem
):
    grids = both_ref.shape[0] // 2
    fetch = pltpu.make_async_copy(got_ref.at[0:HEAD, :], head, sem)
    fetch.start()
    own = jnp.int32(HEAD)
    for i in range(grids):
        own = own + (levels_ref[0, i] + 1) * (levels_ref[1, i] + 1) * (levels_ref[2, i] + 1)
    fetch.wait()

    def unpack(i, start):
        rows, stop = positions(head, i, start)
        tiles = owner_tiles(head, i)
        for k in range(TILES):
            tile = packed_tile(got_ref, rows, k)
            other_ref[tile_rows(i, k), :] = jnp.where(tiles[k], tile, 0.0)
        return stop

    stop = over_grids(grids, unpack, jnp.int32(HEAD))
    full_ref[0] = (jnp.maximum(own, stop) > HEAD + ROOM).astype(jnp.int32)
    total = jnp.zeros((2 * grids, 2 * grids), jnp.float32)
    for s in range(0, SUBSPACES, 8):
        at = slice(s * LANES, (s + 8) * LANES)
        total = total + inner(both_ref[:, at], split(other_ref, s, grids))
    folded = block_ref[...] + fold_cross(whole_products(total))
    for k in range(parts_ref.shape[0]):
        parts_ref[k] = folded


def cross_products(levels, both, block, got, copies):
    grids = both.shape[0] // 2
    return pl.pallas_call(
        cross_kernel,
        compiler_params=GRANT,
        out_shape=(
            jax.ShapeDtypeStruct((copies, 8, LANES), jnp.float32),
            jax.ShapeDtypeStruct((1,), jnp.int32),
        ),
        in_specs=[SMEM, VMEM, VMEM, VMEM],
        out_specs=(VMEM, SMEM),
        scratch_shapes=[
            pltpu.VMEM((grids * SUBSPACES, LANES), jnp.float32),
            pltpu.SMEM((HEAD, LANES), jnp.float32),
            pltpu.SemaphoreType.DMA,
        ],
    )(levels, both, block, got)


def eliminate(parts_ref, grids):
    number = 2 * grids
    senders = parts_ref.shape[0] // 2
    first, last = parts_ref[0], parts_ref[senders]
    for k in range(1, senders):
        first = first + parts_ref[k]
        last = last + parts_ref[senders + k]
    gram = unfold(first, last, grids)
    rows = lax.broadcasted_iota(jnp.int32, gram.shape, 0)
    lanes = lax.broadcasted_iota(jnp.int32, gram.shape, 1)
    on_diagonal = rows == lanes
    diagonal = jnp.sum(jnp.where(on_diagonal, gram, 0.0), axis=1, keepdims=True) + 1e-06
    system = gram + jnp.where(on_diagonal, 0.1 * diagonal, 0.0)
    system = jnp.where(lanes == number, diagonal, system)
    for first in range(0, number, 8):
        columns = [
            jnp.broadcast_to(system[:, k : k + 1], system.shape) for k in range(first, first + 8)
        ]
        for j in range(8):
            k = first + j
            inverse = 1.0 / columns[j][k : k + 1, :]
            column = jnp.where(rows == k, 0.0, columns[j])
            system = system - column * (system[k : k + 1, :] * inverse)
            for q in range(j + 1, 8):
                scale = columns[j][first + q : first + q + 1, :] * inverse
                columns[q] = columns[q] - column * scale
    last = jnp.broadcast_to(system[:, number : number + 1], system.shape)
    solved = jnp.where(on_diagonal, last / system, 0.0)
    return jnp.broadcast_to(jnp.sum(solved, axis=1, keepdims=True), system.shape), on_diagonal


def solve_kernel(parts_ref, out_ref):
    solution_rows, on_diagonal = eliminate(parts_ref, out_ref.shape[1] // 2)
    out_ref[...] = jnp.sum(jnp.where(on_diagonal, solution_rows, 0.0), axis=0, keepdims=True)[:, : out_ref.shape[1]]


def solve_parts(parts, grids):
    return pl.pallas_call(
        solve_kernel,
        compiler_params=GRANT,
        out_shape=jax.ShapeDtypeStruct((1, 2 * grids), jnp.float32),
        in_specs=[VMEM],
        out_specs=VMEM,
    )(parts)


def finish_kernel(
    levels_ref,
    parts_ref,
    surplus_ref,
    got_near_ref,
    got_far_ref,
    updated_ref,
    out_ref,
    head,
    head_sem,
    weights,
    result,
    out_sems,
):
    grids = surplus_ref.shape[0]
    side = lax.axis_index("grp")
    fetch = pltpu.make_async_copy(got_near_ref.at[0:HEAD, :], head, head_sem)
    fetch.start()
    solution_rows, on_diagonal = eliminate(parts_ref, grids)
    weights[...] = solution_rows
    out_ref[...] = jnp.sum(jnp.where(on_diagonal, solution_rows, 0.0), axis=0, keepdims=True)[:, : out_ref.shape[1]]
    fetch.wait()

    def add(i, carry):
        start, sums = carry
        rows, stop = positions(head, i, start)
        own_tiles = owner_tiles(levels_ref, i)
        other_tiles = owner_tiles(head, i)
        own = jnp.broadcast_to(weights[pl.ds(side * grids + i, 1), :], (8, LANES))
        other = jnp.broadcast_to(weights[pl.ds((1 - side) * grids + i, 1), :], (8, LANES))
        added = []
        for slot, got in ((0, got_near_ref), (1, got_far_ref)):
            for k in range(TILES):
                mine = jnp.where(own_tiles[k], cell_tile(surplus_ref, i, k, slot), 0.0)
                theirs = jnp.where(other_tiles[k], packed_tile(got, rows, k), 0.0)
                added.append(sums[slot * TILES + k] + own * mine + other * theirs)
        return stop, tuple(added)

    zero = jnp.zeros((8, LANES), jnp.float32)
    _, sums = over_grids(grids, add, (jnp.int32(HEAD), (zero,) * (2 * TILES)))

    def put(i, slot):
        rows = pl.ds(i * SUBSPACES, SUBSPACES)
        return pltpu.make_async_copy(result.at[slot, rows, :], updated_ref.at[i, :, half_lanes(slot)], out_sems.at[slot, i])

    def spread(i, carry):
        tiles = owner_tiles(levels_ref, i)
        for slot in range(2):
            for k in range(TILES):
                result[slot, tile_rows(i, k), :] = jnp.where(tiles[k], sums[slot * TILES + k], 0.0)
            put(i, slot).start()
        return carry

    over_grids(grids, spread, 0)
    for i in range(grids):
        put(i, 0).wait()
        put(i, 1).wait()


def finish(levels, parts, surplus, got_near, got_far):
    grids = surplus.shape[0]
    return pl.pallas_call(
        finish_kernel,
        compiler_params=GRANT,
        out_shape=(
            jax.ShapeDtypeStruct(surplus.shape, jnp.float32),
            jax.ShapeDtypeStruct((1, 2 * grids), jnp.float32),
        ),
        in_specs=[SMEM, VMEM, VMEM, VMEM, VMEM],
        out_specs=(ANY, VMEM),
        scratch_shapes=[
            pltpu.SMEM((HEAD, LANES), jnp.float32),
            pltpu.SemaphoreType.DMA,
            pltpu.VMEM((2 * grids, LANES), jnp.float32),
            pltpu.VMEM((2, grids * SUBSPACES, LANES), jnp.float32),
            pltpu.SemaphoreType.DMA((2, grids)),
        ],
    )(levels, parts, surplus, got_near, got_far)


def owned(levels, count):
    indices = jnp.arange(count, dtype=jnp.int32)
    digits = jnp.stack([indices // 16, indices // 4 % 4, indices % 4])
    return jnp.all(digits[:, None] <= levels[:, :, None], axis=0).astype(jnp.float32)


def halves(levels, surplus):
    second = lax.axis_index("grp") == 1
    masked = surplus * owned(levels, SUBSPACES)[:, :, None]
    low, high = masked[:, :, :LANES], masked[:, :, LANES:]
    return jnp.where(second, high, low), jnp.where(second, low, high)


def dense_finish(levels, surplus):
    grids = surplus.shape[0]
    second = lax.axis_index("grp") == 1
    near, far = halves(levels, surplus)
    got_near = lax.ppermute(far, "grp", SWAP)
    got_far = lax.ppermute(near, "grp", SWAP)

    def products(left, right):
        return lax.dot_general(
            left,
            right,
            (((1, 2), (1, 2)), ((), ())),
            precision=lax.Precision.HIGHEST,
            preferred_element_type=jnp.float32,
        )

    cross = products(near, got_near)
    own = products(near, near) + products(far, far)
    folded = fold_own(own) + fold_cross(cross)
    pair = jnp.stack([jnp.where(second, 0.0, folded), jnp.where(second, folded, 0.0)])
    for axis in ("grp", *DOM):
        pair = lax.psum(pair, axis)
    coefficients = solve_parts(pair, grids)
    start, stop = coefficients[0, :grids], coefficients[0, grids:]
    own = jnp.where(second, stop, start)[:, None, None]
    other = jnp.where(second, start, stop)[:, None, None]
    sum_near = jnp.sum(own * near + other * got_near, axis=0)
    sum_far = jnp.sum(own * far + other * got_far, axis=0)
    combined = jnp.concatenate(
        [jnp.where(second, sum_far, sum_near), jnp.where(second, sum_near, sum_far)], axis=1
    )
    return owned(levels, SUBSPACES)[:, :, None] * combined[None], coefficients


def exchanged(copies, axes):
    return lax.all_to_all(copies, axes, split_axis=0, concat_axis=0, tiled=True)


def whole(surplus, levels):
    levels = levels.T
    far = pack_far(levels, surplus)
    got_near = lax.ppermute(far, "grp", SWAP)
    near = pack_near(levels, surplus)
    got_far = lax.ppermute(near, "grp", SWAP)
    both, block = own_products(levels, surplus)
    parts, full = cross_products(levels, both, block, got_near, lax.axis_size(STAGES[0]))
    for axes, following in zip(STAGES, STAGES[1:]):
        folded = jnp.sum(exchanged(parts, axes), axis=0)
        parts = jnp.broadcast_to(folded, (lax.axis_size(following), *folded.shape))
    parts = exchanged(parts, STAGES[-1])
    updated, coefficients = lax.cond(
        full[0] > 0,
        lambda: dense_finish(levels, surplus),
        lambda: tuple(finish(levels, parts, surplus, got_near, got_far)),
    )
    return updated, coefficients.reshape(-1)


def solution(mesh):
    torus = Mesh(
        mesh.devices.reshape(mesh.shape["grp"], 8, 8, 2, 2),
        ("grp", *DOM),
    )
    return jax.shard_map(
        whole,
        mesh=torus,
        in_specs=(P("grp", None, DOM), P("grp", None)),
        out_specs=(P("grp", None, DOM), P()),
        check_vma=False,
    )
```

```python
import jax
import jax.numpy as jnp
from jax import lax
from jax.experimental import pallas as pl
from jax.experimental.pallas import tpu as pltpu
from jax.sharding import Mesh
from jax.sharding import PartitionSpec as P

DOM = ("z", "y", "x_hi", "core")
WIDE = ("grp", "y", "x_hi", "core")
SWAP = ((0, 1), (1, 0))
LANES = 128
SUBSPACES = 64
TILES = 8
HEAD = 8
ROOM = 576
ROWS = HEAD + ROOM + 24
VMEM = pl.BlockSpec(memory_space=pltpu.VMEM)
SMEM = pl.BlockSpec(memory_space=pltpu.SMEM)
ANY = pl.BlockSpec(memory_space=pl.ANY)
GRANT = pltpu.CompilerParams(vmem_limit_bytes=12 << 20)


def positions(levels, i, start):
    l0, l1, l2 = (levels[d, i].astype(jnp.int32) for d in range(3))
    width = l2 + 1
    block = (l1 + 1) * width
    rows = []
    at = start
    for _ in range(4):
        base = jnp.minimum(at, HEAD + ROOM)
        rows += [base, base + width, base + 2 * width, base + 3 * width]
        at = at + block
    return rows, start + (l0 + 1) * block


def owner_tiles(levels, i):
    l0, l1, l2 = (levels[d, i].astype(jnp.int32) for d in range(3))
    row = lax.broadcasted_iota(jnp.int32, (8, LANES), 0)
    fits = (row & 3) <= l2
    return [fits & (k % 2 * 2 + (row >> 2) <= l1) & (k // 2 <= l0) for k in range(TILES)]


def tile_rows(i, k):
    return pl.ds(pl.multiple_of(i * SUBSPACES + k * 8, 8), 8)


def packed_tile(packed_ref, rows, k):
    row = lax.broadcasted_iota(jnp.int32, (8, LANES), 0)
    upper = packed_ref[pl.ds(rows[2 * k], 8), :]
    lower = packed_ref[pl.ds(rows[2 * k + 1] - 4, 8), :]
    return jnp.where(row < 4, upper, lower)


def half_lanes(slot):
    side = lax.axis_index("grp")
    return pl.ds(pl.multiple_of((1 - side if slot else side) * LANES, LANES), LANES)


def cell_tile(surplus_ref, i, k, slot):
    return surplus_ref[i, k * 8 : k * 8 + 8, half_lanes(slot)]


def store_packed(out_ref, rows, k, tile):
    out_ref[pl.ds(rows[2 * k], 4), :] = tile[0:4]
    out_ref[pl.ds(rows[2 * k + 1], 4), :] = tile[4:8]


def pack_far_kernel(levels_ref, surplus_ref, out_ref, held, sems):
    grids = surplus_ref.shape[0]

    def copy(i):
        rows = pl.ds(i * SUBSPACES, SUBSPACES)
        return pltpu.make_async_copy(surplus_ref.at[i, :, half_lanes(1)], held.at[rows, :], sems.at[i])

    for i in range(grids):
        copy(i).start()
    head = jnp.zeros((HEAD, LANES), jnp.float32)
    row = lax.broadcasted_iota(jnp.int32, head.shape, 0)
    lane = lax.broadcasted_iota(jnp.int32, head.shape, 1)
    for d in range(3):
        for i in range(grids):
            head = jnp.where((row == d) & (lane == i), levels_ref[d, i].astype(jnp.float32), head)
    out_ref[0:HEAD, :] = head

    def pack(i, start):
        copy(i).wait()
        rows, stop = positions(levels_ref, i, start)
        for k in range(TILES):
            store_packed(out_ref, rows, k, held[tile_rows(i, k), :])
        return stop

    over_grids(grids, pack, jnp.int32(HEAD))


def pack_far(levels, surplus):
    grids = surplus.shape[0]
    return pl.pallas_call(
        pack_far_kernel,
        compiler_params=GRANT,
        out_shape=jax.ShapeDtypeStruct((ROWS, LANES), jnp.float32),
        in_specs=[SMEM, ANY],
        out_specs=VMEM,
        scratch_shapes=[
            pltpu.VMEM((grids * SUBSPACES, LANES), jnp.float32),
            pltpu.SemaphoreType.DMA((grids,)),
        ],
    )(levels, surplus)


def pack_near_kernel(levels_ref, surplus_ref, out_ref):
    grids = surplus_ref.shape[0]
    out_ref[0:HEAD, :] = jnp.zeros((HEAD, LANES), jnp.float32)

    def pack(i, start):
        rows, stop = positions(levels_ref, i, start)
        for k in range(TILES):
            store_packed(out_ref, rows, k, cell_tile(surplus_ref, i, k, 0))
        return stop

    over_grids(grids, pack, jnp.int32(HEAD))


def pack_near(levels, surplus):
    return pl.pallas_call(
        pack_near_kernel,
        compiler_params=GRANT,
        out_shape=jax.ShapeDtypeStruct((ROWS, LANES), jnp.float32),
        in_specs=[SMEM, VMEM],
        out_specs=VMEM,
    )(levels, surplus)


def over_grids(grids, body, init):
    def step(n, carry):
        return body(2 * n + 1, body(2 * n, carry))

    return lax.fori_loop(0, grids // 2, step, init)


def split(ref, s, grids):
    rows = [ref[pl.ds(s + k, grids, stride=SUBSPACES), :] for k in range(8)]
    rows = jnp.concatenate(rows, axis=1)
    high = rows.astype(jnp.bfloat16).astype(jnp.float32)
    return jnp.concatenate([high, rows - high], axis=0).astype(jnp.bfloat16)


def inner(left, right):
    return lax.dot_general(
        left, right, (((1,), (1,)), ((), ())), preferred_element_type=jnp.float32
    )


def whole_products(total):
    grids = total.shape[0] // 2
    rows = total[:grids, :] + total[grids:, :]
    return rows[:, :grids] + rows[:, grids:]


def own_kernel(levels_ref, surplus_ref, both_ref, block_ref, near_ref, far_ref):
    grids = surplus_ref.shape[0]

    def mask(i, carry):
        tiles = owner_tiles(levels_ref, i)
        for k in range(TILES):
            at = tile_rows(i, k)
            near_ref[at, :] = jnp.where(tiles[k], cell_tile(surplus_ref, i, k, 0), 0.0)
            far_ref[at, :] = jnp.where(tiles[k], cell_tile(surplus_ref, i, k, 1), 0.0)
        return carry

    over_grids(grids, mask, 0)
    total = jnp.zeros((2 * grids, 2 * grids), jnp.float32)
    for s in range(0, SUBSPACES, 8):
        near = split(near_ref, s, grids)
        far = split(far_ref, s, grids)
        both_ref[:, s * LANES : (s + 8) * LANES] = near
        total = total + inner(near, near) + inner(far, far)
    block_ref[...] = fold_own(whole_products(total))


def own_products(levels, surplus):
    grids = surplus.shape[0]
    both = jax.ShapeDtypeStruct((2 * grids, SUBSPACES * LANES), jnp.bfloat16)
    half = pltpu.VMEM((grids * SUBSPACES, LANES), jnp.float32)
    return pl.pallas_call(
        own_kernel,
        compiler_params=GRANT,
        out_shape=(both, jax.ShapeDtypeStruct((8, LANES), jnp.float32)),
        in_specs=[SMEM, VMEM],
        out_specs=(VMEM, VMEM),
        scratch_shapes=[half, half],
    )(levels, surplus)


def fold_own(block):
    strips = [block[r : r + 8, r:] for r in range(0, block.shape[0], 8)]
    used = sum(strip.shape[1] for strip in strips)
    return jnp.concatenate([*strips, jnp.zeros((8, LANES - used), jnp.float32)], axis=1)


def fold_cross(cross):
    grids = cross.shape[0]
    strips = [cross[r : r + 8, :] for r in range(0, grids, 8)]
    ahead = sum(range(8, grids + 8, 8))
    behind = LANES - ahead - grids * len(strips)
    zeros = [jnp.zeros((8, width), jnp.float32) for width in (ahead, behind)]
    return jnp.concatenate([zeros[0], *strips, zeros[1]], axis=1)


def unfold(first, last, grids):
    def strips(folded):
        own, at = [], 0
        for r in range(0, grids, 8):
            strip = folded[:, at : at + grids - r]
            own.append(jnp.concatenate([jnp.zeros((8, r), jnp.float32), strip], axis=1) if r else strip)
            at += grids - r
        cross = [folded[:, at + n * grids : at + (n + 1) * grids] for n in range(grids // 8)]
        return own, cross

    own_first, cross_first = strips(first)
    own_last, cross_last = strips(last)
    half = jnp.concatenate(
        [jnp.concatenate(pair, axis=1) for pair in zip(own_first, cross_first)]
        + [jnp.concatenate(pair, axis=1) for pair in zip(cross_last, own_last)],
        axis=0,
    )
    turned = half.T
    rows = lax.broadcasted_iota(jnp.int32, half.shape, 0)
    columns = lax.broadcasted_iota(jnp.int32, half.shape, 1)
    between = (rows < grids) != (columns < grids)
    gram = jnp.where(rows >> 3 <= columns >> 3, half, turned)
    gram = jnp.where(between, half + turned, gram)
    return jnp.concatenate([gram, jnp.zeros((2 * grids, LANES - 2 * grids), jnp.float32)], axis=1)


def cross_kernel(
    levels_ref, both_ref, block_ref, got_ref, parts_ref, full_ref, other_ref, head, sem
):
    grids = both_ref.shape[0] // 2
    fetch = pltpu.make_async_copy(got_ref.at[0:HEAD, :], head, sem)
    fetch.start()
    own = jnp.int32(HEAD)
    for i in range(grids):
        own = own + (levels_ref[0, i] + 1) * (levels_ref[1, i] + 1) * (levels_ref[2, i] + 1)
    fetch.wait()

    def unpack(i, start):
        rows, stop = positions(head, i, start)
        tiles = owner_tiles(head, i)
        for k in range(TILES):
            tile = packed_tile(got_ref, rows, k)
            other_ref[tile_rows(i, k), :] = jnp.where(tiles[k], tile, 0.0)
        return stop

    stop = over_grids(grids, unpack, jnp.int32(HEAD))
    full_ref[0] = (jnp.maximum(own, stop) > HEAD + ROOM).astype(jnp.int32)
    total = jnp.zeros((2 * grids, 2 * grids), jnp.float32)
    for s in range(0, SUBSPACES, 8):
        at = slice(s * LANES, (s + 8) * LANES)
        total = total + inner(both_ref[:, at], split(other_ref, s, grids))
    folded = block_ref[...] + fold_cross(whole_products(total))
    for k in range(parts_ref.shape[0]):
        parts_ref[k] = folded


def cross_products(levels, both, block, got, copies):
    grids = both.shape[0] // 2
    return pl.pallas_call(
        cross_kernel,
        compiler_params=GRANT,
        out_shape=(
            jax.ShapeDtypeStruct((copies, 8, LANES), jnp.float32),
            jax.ShapeDtypeStruct((1,), jnp.int32),
        ),
        in_specs=[SMEM, VMEM, VMEM, VMEM],
        out_specs=(VMEM, SMEM),
        scratch_shapes=[
            pltpu.VMEM((grids * SUBSPACES, LANES), jnp.float32),
            pltpu.SMEM((HEAD, LANES), jnp.float32),
            pltpu.SemaphoreType.DMA,
        ],
    )(levels, both, block, got)


def eliminate(parts_ref, grids):
    number = 2 * grids
    first, last = parts_ref[0, 0], parts_ref[0, 1]
    for k in range(1, parts_ref.shape[0]):
        first = first + parts_ref[k, 0]
        last = last + parts_ref[k, 1]
    gram = unfold(first, last, grids)
    rows = lax.broadcasted_iota(jnp.int32, gram.shape, 0)
    lanes = lax.broadcasted_iota(jnp.int32, gram.shape, 1)
    on_diagonal = rows == lanes
    diagonal = jnp.sum(jnp.where(on_diagonal, gram, 0.0), axis=1, keepdims=True) + 1e-06
    system = gram + jnp.where(on_diagonal, 0.1 * diagonal, 0.0)
    system = jnp.where(lanes == number, diagonal, system)
    for first in range(0, number, 8):
        columns = [
            jnp.broadcast_to(system[:, k : k + 1], system.shape) for k in range(first, first + 8)
        ]
        for j in range(8):
            k = first + j
            inverse = 1.0 / columns[j][k : k + 1, :]
            column = jnp.where(rows == k, 0.0, columns[j])
            system = system - column * (system[k : k + 1, :] * inverse)
            for q in range(j + 1, 8):
                scale = columns[j][first + q : first + q + 1, :] * inverse
                columns[q] = columns[q] - column * scale
    last = jnp.broadcast_to(system[:, number : number + 1], system.shape)
    solved = jnp.where(on_diagonal, last / system, 0.0)
    return jnp.broadcast_to(jnp.sum(solved, axis=1, keepdims=True), system.shape), on_diagonal


def solve_kernel(parts_ref, out_ref):
    solution_rows, on_diagonal = eliminate(parts_ref, out_ref.shape[1] // 2)
    out_ref[...] = jnp.sum(jnp.where(on_diagonal, solution_rows, 0.0), axis=0, keepdims=True)[:, : out_ref.shape[1]]


def solve_parts(parts, grids):
    return pl.pallas_call(
        solve_kernel,
        compiler_params=GRANT,
        out_shape=jax.ShapeDtypeStruct((1, 2 * grids), jnp.float32),
        in_specs=[VMEM],
        out_specs=VMEM,
    )(parts)


def finish_kernel(
    levels_ref,
    parts_ref,
    surplus_ref,
    got_near_ref,
    got_far_ref,
    updated_ref,
    out_ref,
    head,
    head_sem,
    weights,
    result,
    out_sems,
):
    grids = surplus_ref.shape[0]
    side = lax.axis_index("grp")
    fetch = pltpu.make_async_copy(got_near_ref.at[0:HEAD, :], head, head_sem)
    fetch.start()
    solution_rows, on_diagonal = eliminate(parts_ref, grids)
    weights[...] = solution_rows
    out_ref[...] = jnp.sum(jnp.where(on_diagonal, solution_rows, 0.0), axis=0, keepdims=True)[:, : out_ref.shape[1]]
    fetch.wait()

    def add(i, carry):
        start, sums = carry
        rows, stop = positions(head, i, start)
        own_tiles = owner_tiles(levels_ref, i)
        other_tiles = owner_tiles(head, i)
        own = jnp.broadcast_to(weights[pl.ds(side * grids + i, 1), :], (8, LANES))
        other = jnp.broadcast_to(weights[pl.ds((1 - side) * grids + i, 1), :], (8, LANES))
        added = []
        for slot, got in ((0, got_near_ref), (1, got_far_ref)):
            for k in range(TILES):
                mine = jnp.where(own_tiles[k], cell_tile(surplus_ref, i, k, slot), 0.0)
                theirs = jnp.where(other_tiles[k], packed_tile(got, rows, k), 0.0)
                added.append(sums[slot * TILES + k] + own * mine + other * theirs)
        return stop, tuple(added)

    zero = jnp.zeros((8, LANES), jnp.float32)
    _, sums = over_grids(grids, add, (jnp.int32(HEAD), (zero,) * (2 * TILES)))

    def put(i, slot):
        rows = pl.ds(i * SUBSPACES, SUBSPACES)
        return pltpu.make_async_copy(result.at[slot, rows, :], updated_ref.at[i, :, half_lanes(slot)], out_sems.at[slot, i])

    def spread(i, carry):
        tiles = owner_tiles(levels_ref, i)
        for slot in range(2):
            for k in range(TILES):
                result[slot, tile_rows(i, k), :] = jnp.where(tiles[k], sums[slot * TILES + k], 0.0)
            put(i, slot).start()
        return carry

    over_grids(grids, spread, 0)
    for i in range(grids):
        put(i, 0).wait()
        put(i, 1).wait()


def finish(levels, parts, surplus, got_near, got_far):
    grids = surplus.shape[0]
    return pl.pallas_call(
        finish_kernel,
        compiler_params=GRANT,
        out_shape=(
            jax.ShapeDtypeStruct(surplus.shape, jnp.float32),
            jax.ShapeDtypeStruct((1, 2 * grids), jnp.float32),
        ),
        in_specs=[SMEM, VMEM, VMEM, VMEM, VMEM],
        out_specs=(ANY, VMEM),
        scratch_shapes=[
            pltpu.SMEM((HEAD, LANES), jnp.float32),
            pltpu.SemaphoreType.DMA,
            pltpu.VMEM((2 * grids, LANES), jnp.float32),
            pltpu.VMEM((2, grids * SUBSPACES, LANES), jnp.float32),
            pltpu.SemaphoreType.DMA((2, grids)),
        ],
    )(levels, parts, surplus, got_near, got_far)


def owned(levels, count):
    indices = jnp.arange(count, dtype=jnp.int32)
    digits = jnp.stack([indices // 16, indices // 4 % 4, indices % 4])
    return jnp.all(digits[:, None] <= levels[:, :, None], axis=0).astype(jnp.float32)


def halves(levels, surplus):
    second = lax.axis_index("grp") == 1
    masked = surplus * owned(levels, SUBSPACES)[:, :, None]
    low, high = masked[:, :, :LANES], masked[:, :, LANES:]
    return jnp.where(second, high, low), jnp.where(second, low, high)


def dense_finish(levels, surplus):
    grids = surplus.shape[0]
    second = lax.axis_index("grp") == 1
    near, far = halves(levels, surplus)
    got_near = lax.ppermute(far, "grp", SWAP)
    got_far = lax.ppermute(near, "grp", SWAP)

    def products(left, right):
        return lax.dot_general(
            left,
            right,
            (((1, 2), (1, 2)), ((), ())),
            precision=lax.Precision.HIGHEST,
            preferred_element_type=jnp.float32,
        )

    cross = products(near, got_near)
    own = products(near, near) + products(far, far)
    folded = fold_own(own) + fold_cross(cross)
    pair = jnp.stack([jnp.where(second, 0.0, folded), jnp.where(second, folded, 0.0)])
    for axis in ("grp", *DOM):
        pair = lax.psum(pair, axis)
    coefficients = solve_parts(pair[None], grids)
    start, stop = coefficients[0, :grids], coefficients[0, grids:]
    own = jnp.where(second, stop, start)[:, None, None]
    other = jnp.where(second, start, stop)[:, None, None]
    sum_near = jnp.sum(own * near + other * got_near, axis=0)
    sum_far = jnp.sum(own * far + other * got_far, axis=0)
    combined = jnp.concatenate(
        [jnp.where(second, sum_far, sum_near), jnp.where(second, sum_near, sum_far)], axis=1
    )
    return owned(levels, SUBSPACES)[:, :, None] * combined[None], coefficients


def exchanged(copies, axes):
    return lax.all_to_all(copies, axes, split_axis=0, concat_axis=0, tiled=True)


def whole(surplus, levels):
    levels = levels.T
    far = pack_far(levels, surplus)
    got_near = lax.ppermute(far, "grp", SWAP)
    near = pack_near(levels, surplus)
    got_far = lax.ppermute(near, "grp", SWAP)
    both, block = own_products(levels, surplus)
    parts, full = cross_products(levels, both, block, got_near, lax.axis_size(WIDE))
    parts = exchanged(parts, WIDE)
    sums = jnp.sum(parts.reshape(2, -1, *parts.shape[1:]), axis=1)
    parts = exchanged(jnp.broadcast_to(sums, (lax.axis_size("z"), *sums.shape)), "z")
    updated, coefficients = lax.cond(
        full[0] > 0,
        lambda: dense_finish(levels, surplus),
        lambda: tuple(finish(levels, parts, surplus, got_near, got_far)),
    )
    return updated, coefficients.reshape(-1)


def solution(mesh):
    torus = Mesh(
        mesh.devices.reshape(mesh.shape["grp"], 8, 8, 2, 2),
        ("grp", *DOM),
    )
    return jax.shard_map(
        whole,
        mesh=torus,
        in_specs=(P("grp", None, DOM), P("grp", None)),
        out_specs=(P("grp", None, DOM), P()),
        check_vma=False,
    )
```

```python
import jax
import jax.numpy as jnp
from jax import lax
from jax.experimental import pallas as pl
from jax.experimental.pallas import tpu as pltpu
from jax.sharding import Mesh
from jax.sharding import PartitionSpec as P

DOM = ("z", "y", "x_hi", "core")
WIDE = ("grp", "z", "x_hi", "core")
SWAP = ((0, 1), (1, 0))
LANES = 128
SUBSPACES = 64
TILES = 8
HEAD = 8
ROOM = 576
ROWS = HEAD + ROOM + 24
VMEM = pl.BlockSpec(memory_space=pltpu.VMEM)
SMEM = pl.BlockSpec(memory_space=pltpu.SMEM)
ANY = pl.BlockSpec(memory_space=pl.ANY)
GRANT = pltpu.CompilerParams(vmem_limit_bytes=12 << 20)


def positions(levels, i, start):
    l0, l1, l2 = (levels[d, i].astype(jnp.int32) for d in range(3))
    width = l2 + 1
    block = (l1 + 1) * width
    rows = []
    at = start
    for _ in range(4):
        base = jnp.minimum(at, HEAD + ROOM)
        rows += [base, base + width, base + 2 * width, base + 3 * width]
        at = at + block
    return rows, start + (l0 + 1) * block


def owner_tiles(levels, i):
    l0, l1, l2 = (levels[d, i].astype(jnp.int32) for d in range(3))
    row = lax.broadcasted_iota(jnp.int32, (8, LANES), 0)
    fits = (row & 3) <= l2
    return [fits & (k % 2 * 2 + (row >> 2) <= l1) & (k // 2 <= l0) for k in range(TILES)]


def tile_rows(i, k):
    return pl.ds(pl.multiple_of(i * SUBSPACES + k * 8, 8), 8)


def packed_tile(packed_ref, rows, k):
    row = lax.broadcasted_iota(jnp.int32, (8, LANES), 0)
    upper = packed_ref[pl.ds(rows[2 * k], 8), :]
    lower = packed_ref[pl.ds(rows[2 * k + 1] - 4, 8), :]
    return jnp.where(row < 4, upper, lower)


def half_lanes(slot):
    side = lax.axis_index("grp")
    return pl.ds(pl.multiple_of((1 - side if slot else side) * LANES, LANES), LANES)


def cell_tile(surplus_ref, i, k, slot):
    return surplus_ref[i, k * 8 : k * 8 + 8, half_lanes(slot)]


def store_packed(out_ref, rows, k, tile):
    out_ref[pl.ds(rows[2 * k], 4), :] = tile[0:4]
    out_ref[pl.ds(rows[2 * k + 1], 4), :] = tile[4:8]


def pack_far_kernel(levels_ref, surplus_ref, out_ref, held, sems):
    grids = surplus_ref.shape[0]

    def copy(i):
        rows = pl.ds(i * SUBSPACES, SUBSPACES)
        return pltpu.make_async_copy(surplus_ref.at[i, :, half_lanes(1)], held.at[rows, :], sems.at[i])

    for i in range(grids):
        copy(i).start()
    head = jnp.zeros((HEAD, LANES), jnp.float32)
    row = lax.broadcasted_iota(jnp.int32, head.shape, 0)
    lane = lax.broadcasted_iota(jnp.int32, head.shape, 1)
    for d in range(3):
        for i in range(grids):
            head = jnp.where((row == d) & (lane == i), levels_ref[d, i].astype(jnp.float32), head)
    out_ref[0:HEAD, :] = head

    def pack(i, start):
        copy(i).wait()
        rows, stop = positions(levels_ref, i, start)
        for k in range(TILES):
            store_packed(out_ref, rows, k, held[tile_rows(i, k), :])
        return stop

    over_grids(grids, pack, jnp.int32(HEAD))


def pack_far(levels, surplus):
    grids = surplus.shape[0]
    return pl.pallas_call(
        pack_far_kernel,
        compiler_params=GRANT,
        out_shape=jax.ShapeDtypeStruct((ROWS, LANES), jnp.float32),
        in_specs=[SMEM, ANY],
        out_specs=VMEM,
        scratch_shapes=[
            pltpu.VMEM((grids * SUBSPACES, LANES), jnp.float32),
            pltpu.SemaphoreType.DMA((grids,)),
        ],
    )(levels, surplus)


def pack_near_kernel(levels_ref, surplus_ref, out_ref):
    grids = surplus_ref.shape[0]
    out_ref[0:HEAD, :] = jnp.zeros((HEAD, LANES), jnp.float32)

    def pack(i, start):
        rows, stop = positions(levels_ref, i, start)
        for k in range(TILES):
            store_packed(out_ref, rows, k, cell_tile(surplus_ref, i, k, 0))
        return stop

    over_grids(grids, pack, jnp.int32(HEAD))


def pack_near(levels, surplus):
    return pl.pallas_call(
        pack_near_kernel,
        compiler_params=GRANT,
        out_shape=jax.ShapeDtypeStruct((ROWS, LANES), jnp.float32),
        in_specs=[SMEM, VMEM],
        out_specs=VMEM,
    )(levels, surplus)


def over_grids(grids, body, init):
    def step(n, carry):
        return body(2 * n + 1, body(2 * n, carry))

    return lax.fori_loop(0, grids // 2, step, init)


def split(ref, s, grids):
    rows = [ref[pl.ds(s + k, grids, stride=SUBSPACES), :] for k in range(8)]
    rows = jnp.concatenate(rows, axis=1)
    high = rows.astype(jnp.bfloat16).astype(jnp.float32)
    return jnp.concatenate([high, rows - high], axis=0).astype(jnp.bfloat16)


def inner(left, right):
    return lax.dot_general(
        left, right, (((1,), (1,)), ((), ())), preferred_element_type=jnp.float32
    )


def whole_products(total):
    grids = total.shape[0] // 2
    rows = total[:grids, :] + total[grids:, :]
    return rows[:, :grids] + rows[:, grids:]


def own_kernel(levels_ref, surplus_ref, both_ref, block_ref, near_ref, far_ref):
    grids = surplus_ref.shape[0]

    def mask(i, carry):
        tiles = owner_tiles(levels_ref, i)
        for k in range(TILES):
            at = tile_rows(i, k)
            near_ref[at, :] = jnp.where(tiles[k], cell_tile(surplus_ref, i, k, 0), 0.0)
            far_ref[at, :] = jnp.where(tiles[k], cell_tile(surplus_ref, i, k, 1), 0.0)
        return carry

    over_grids(grids, mask, 0)
    total = jnp.zeros((2 * grids, 2 * grids), jnp.float32)
    for s in range(0, SUBSPACES, 8):
        near = split(near_ref, s, grids)
        far = split(far_ref, s, grids)
        both_ref[:, s * LANES : (s + 8) * LANES] = near
        total = total + inner(near, near) + inner(far, far)
    block_ref[...] = fold_own(whole_products(total))


def own_products(levels, surplus):
    grids = surplus.shape[0]
    both = jax.ShapeDtypeStruct((2 * grids, SUBSPACES * LANES), jnp.bfloat16)
    half = pltpu.VMEM((grids * SUBSPACES, LANES), jnp.float32)
    return pl.pallas_call(
        own_kernel,
        compiler_params=GRANT,
        out_shape=(both, jax.ShapeDtypeStruct((8, LANES), jnp.float32)),
        in_specs=[SMEM, VMEM],
        out_specs=(VMEM, VMEM),
        scratch_shapes=[half, half],
    )(levels, surplus)


def fold_own(block):
    strips = [block[r : r + 8, r:] for r in range(0, block.shape[0], 8)]
    used = sum(strip.shape[1] for strip in strips)
    return jnp.concatenate([*strips, jnp.zeros((8, LANES - used), jnp.float32)], axis=1)


def fold_cross(cross):
    grids = cross.shape[0]
    strips = [cross[r : r + 8, :] for r in range(0, grids, 8)]
    ahead = sum(range(8, grids + 8, 8))
    behind = LANES - ahead - grids * len(strips)
    zeros = [jnp.zeros((8, width), jnp.float32) for width in (ahead, behind)]
    return jnp.concatenate([zeros[0], *strips, zeros[1]], axis=1)


def unfold(first, last, grids):
    def strips(folded):
        own, at = [], 0
        for r in range(0, grids, 8):
            strip = folded[:, at : at + grids - r]
            own.append(jnp.concatenate([jnp.zeros((8, r), jnp.float32), strip], axis=1) if r else strip)
            at += grids - r
        cross = [folded[:, at + n * grids : at + (n + 1) * grids] for n in range(grids // 8)]
        return own, cross

    own_first, cross_first = strips(first)
    own_last, cross_last = strips(last)
    half = jnp.concatenate(
        [jnp.concatenate(pair, axis=1) for pair in zip(own_first, cross_first)]
        + [jnp.concatenate(pair, axis=1) for pair in zip(cross_last, own_last)],
        axis=0,
    )
    turned = half.T
    rows = lax.broadcasted_iota(jnp.int32, half.shape, 0)
    columns = lax.broadcasted_iota(jnp.int32, half.shape, 1)
    between = (rows < grids) != (columns < grids)
    gram = jnp.where(rows >> 3 <= columns >> 3, half, turned)
    gram = jnp.where(between, half + turned, gram)
    return jnp.concatenate([gram, jnp.zeros((2 * grids, LANES - 2 * grids), jnp.float32)], axis=1)


def cross_kernel(
    levels_ref, both_ref, block_ref, got_ref, parts_ref, full_ref, other_ref, head, sem
):
    grids = both_ref.shape[0] // 2
    fetch = pltpu.make_async_copy(got_ref.at[0:HEAD, :], head, sem)
    fetch.start()
    own = jnp.int32(HEAD)
    for i in range(grids):
        own = own + (levels_ref[0, i] + 1) * (levels_ref[1, i] + 1) * (levels_ref[2, i] + 1)
    fetch.wait()

    def unpack(i, start):
        rows, stop = positions(head, i, start)
        tiles = owner_tiles(head, i)
        for k in range(TILES):
            tile = packed_tile(got_ref, rows, k)
            other_ref[tile_rows(i, k), :] = jnp.where(tiles[k], tile, 0.0)
        return stop

    stop = over_grids(grids, unpack, jnp.int32(HEAD))
    full_ref[0] = (jnp.maximum(own, stop) > HEAD + ROOM).astype(jnp.int32)
    total = jnp.zeros((2 * grids, 2 * grids), jnp.float32)
    for s in range(0, SUBSPACES, 8):
        at = slice(s * LANES, (s + 8) * LANES)
        total = total + inner(both_ref[:, at], split(other_ref, s, grids))
    folded = block_ref[...] + fold_cross(whole_products(total))
    for k in range(parts_ref.shape[0]):
        parts_ref[k] = folded


def cross_products(levels, both, block, got, copies):
    grids = both.shape[0] // 2
    return pl.pallas_call(
        cross_kernel,
        compiler_params=GRANT,
        out_shape=(
            jax.ShapeDtypeStruct((copies, 8, LANES), jnp.float32),
            jax.ShapeDtypeStruct((1,), jnp.int32),
        ),
        in_specs=[SMEM, VMEM, VMEM, VMEM],
        out_specs=(VMEM, SMEM),
        scratch_shapes=[
            pltpu.VMEM((grids * SUBSPACES, LANES), jnp.float32),
            pltpu.SMEM((HEAD, LANES), jnp.float32),
            pltpu.SemaphoreType.DMA,
        ],
    )(levels, both, block, got)


def eliminate(parts_ref, grids):
    number = 2 * grids
    first, last = parts_ref[0, 0], parts_ref[0, 1]
    for k in range(1, parts_ref.shape[0]):
        first = first + parts_ref[k, 0]
        last = last + parts_ref[k, 1]
    gram = unfold(first, last, grids)
    rows = lax.broadcasted_iota(jnp.int32, gram.shape, 0)
    lanes = lax.broadcasted_iota(jnp.int32, gram.shape, 1)
    on_diagonal = rows == lanes
    diagonal = jnp.sum(jnp.where(on_diagonal, gram, 0.0), axis=1, keepdims=True) + 1e-06
    system = gram + jnp.where(on_diagonal, 0.1 * diagonal, 0.0)
    system = jnp.where(lanes == number, diagonal, system)
    for first in range(0, number, 8):
        columns = [
            jnp.broadcast_to(system[:, k : k + 1], system.shape) for k in range(first, first + 8)
        ]
        for j in range(8):
            k = first + j
            inverse = 1.0 / columns[j][k : k + 1, :]
            column = jnp.where(rows == k, 0.0, columns[j])
            system = system - column * (system[k : k + 1, :] * inverse)
            for q in range(j + 1, 8):
                scale = columns[j][first + q : first + q + 1, :] * inverse
                columns[q] = columns[q] - column * scale
    last = jnp.broadcast_to(system[:, number : number + 1], system.shape)
    solved = jnp.where(on_diagonal, last / system, 0.0)
    return jnp.broadcast_to(jnp.sum(solved, axis=1, keepdims=True), system.shape), on_diagonal


def solve_kernel(parts_ref, out_ref):
    solution_rows, on_diagonal = eliminate(parts_ref, out_ref.shape[1] // 2)
    out_ref[...] = jnp.sum(jnp.where(on_diagonal, solution_rows, 0.0), axis=0, keepdims=True)[:, : out_ref.shape[1]]


def solve_parts(parts, grids):
    return pl.pallas_call(
        solve_kernel,
        compiler_params=GRANT,
        out_shape=jax.ShapeDtypeStruct((1, 2 * grids), jnp.float32),
        in_specs=[VMEM],
        out_specs=VMEM,
    )(parts)


def finish_kernel(
    levels_ref,
    parts_ref,
    surplus_ref,
    got_near_ref,
    got_far_ref,
    updated_ref,
    out_ref,
    head,
    head_sem,
    weights,
    result,
    out_sems,
):
    grids = surplus_ref.shape[0]
    side = lax.axis_index("grp")
    fetch = pltpu.make_async_copy(got_near_ref.at[0:HEAD, :], head, head_sem)
    fetch.start()
    solution_rows, on_diagonal = eliminate(parts_ref, grids)
    weights[...] = solution_rows
    out_ref[...] = jnp.sum(jnp.where(on_diagonal, solution_rows, 0.0), axis=0, keepdims=True)[:, : out_ref.shape[1]]
    fetch.wait()

    def add(i, carry):
        start, sums = carry
        rows, stop = positions(head, i, start)
        own_tiles = owner_tiles(levels_ref, i)
        other_tiles = owner_tiles(head, i)
        own = jnp.broadcast_to(weights[pl.ds(side * grids + i, 1), :], (8, LANES))
        other = jnp.broadcast_to(weights[pl.ds((1 - side) * grids + i, 1), :], (8, LANES))
        added = []
        for slot, got in ((0, got_near_ref), (1, got_far_ref)):
            for k in range(TILES):
                mine = jnp.where(own_tiles[k], cell_tile(surplus_ref, i, k, slot), 0.0)
                theirs = jnp.where(other_tiles[k], packed_tile(got, rows, k), 0.0)
                added.append(sums[slot * TILES + k] + own * mine + other * theirs)
        return stop, tuple(added)

    zero = jnp.zeros((8, LANES), jnp.float32)
    _, sums = over_grids(grids, add, (jnp.int32(HEAD), (zero,) * (2 * TILES)))

    def put(i, slot):
        rows = pl.ds(i * SUBSPACES, SUBSPACES)
        return pltpu.make_async_copy(result.at[slot, rows, :], updated_ref.at[i, :, half_lanes(slot)], out_sems.at[slot, i])

    def spread(i, carry):
        tiles = owner_tiles(levels_ref, i)
        for slot in range(2):
            for k in range(TILES):
                result[slot, tile_rows(i, k), :] = jnp.where(tiles[k], sums[slot * TILES + k], 0.0)
            put(i, slot).start()
        return carry

    over_grids(grids, spread, 0)
    for i in range(grids):
        put(i, 0).wait()
        put(i, 1).wait()


def finish(levels, parts, surplus, got_near, got_far):
    grids = surplus.shape[0]
    return pl.pallas_call(
        finish_kernel,
        compiler_params=GRANT,
        out_shape=(
            jax.ShapeDtypeStruct(surplus.shape, jnp.float32),
            jax.ShapeDtypeStruct((1, 2 * grids), jnp.float32),
        ),
        in_specs=[SMEM, VMEM, VMEM, VMEM, VMEM],
        out_specs=(ANY, VMEM),
        scratch_shapes=[
            pltpu.SMEM((HEAD, LANES), jnp.float32),
            pltpu.SemaphoreType.DMA,
            pltpu.VMEM((2 * grids, LANES), jnp.float32),
            pltpu.VMEM((2, grids * SUBSPACES, LANES), jnp.float32),
            pltpu.SemaphoreType.DMA((2, grids)),
        ],
    )(levels, parts, surplus, got_near, got_far)


def owned(levels, count):
    indices = jnp.arange(count, dtype=jnp.int32)
    digits = jnp.stack([indices // 16, indices // 4 % 4, indices % 4])
    return jnp.all(digits[:, None] <= levels[:, :, None], axis=0).astype(jnp.float32)


def halves(levels, surplus):
    second = lax.axis_index("grp") == 1
    masked = surplus * owned(levels, SUBSPACES)[:, :, None]
    low, high = masked[:, :, :LANES], masked[:, :, LANES:]
    return jnp.where(second, high, low), jnp.where(second, low, high)


def dense_finish(levels, surplus):
    grids = surplus.shape[0]
    second = lax.axis_index("grp") == 1
    near, far = halves(levels, surplus)
    got_near = lax.ppermute(far, "grp", SWAP)
    got_far = lax.ppermute(near, "grp", SWAP)

    def products(left, right):
        return lax.dot_general(
            left,
            right,
            (((1, 2), (1, 2)), ((), ())),
            precision=lax.Precision.HIGHEST,
            preferred_element_type=jnp.float32,
        )

    cross = products(near, got_near)
    own = products(near, near) + products(far, far)
    folded = fold_own(own) + fold_cross(cross)
    pair = jnp.stack([jnp.where(second, 0.0, folded), jnp.where(second, folded, 0.0)])
    for axis in ("grp", *DOM):
        pair = lax.psum(pair, axis)
    coefficients = solve_parts(pair[None], grids)
    start, stop = coefficients[0, :grids], coefficients[0, grids:]
    own = jnp.where(second, stop, start)[:, None, None]
    other = jnp.where(second, start, stop)[:, None, None]
    sum_near = jnp.sum(own * near + other * got_near, axis=0)
    sum_far = jnp.sum(own * far + other * got_far, axis=0)
    combined = jnp.concatenate(
        [jnp.where(second, sum_far, sum_near), jnp.where(second, sum_near, sum_far)], axis=1
    )
    return owned(levels, SUBSPACES)[:, :, None] * combined[None], coefficients


def exchanged(copies, axes):
    return lax.all_to_all(copies, axes, split_axis=0, concat_axis=0, tiled=True)


def whole(surplus, levels):
    levels = levels.T
    far = pack_far(levels, surplus)
    got_near = lax.ppermute(far, "grp", SWAP)
    both, block = own_products(levels, surplus)
    later, block = lax.optimization_barrier((levels, block))
    near = pack_near(later, surplus)
    got_far = lax.ppermute(near, "grp", SWAP)
    parts, full = cross_products(levels, both, block, got_near, lax.axis_size(WIDE))
    parts = exchanged(parts, WIDE)
    sums = jnp.sum(parts.reshape(2, -1, *parts.shape[1:]), axis=1)
    parts = exchanged(jnp.broadcast_to(sums, (lax.axis_size("y"), *sums.shape)), "y")
    updated, coefficients = lax.cond(
        full[0] > 0,
        lambda: dense_finish(levels, surplus),
        lambda: tuple(finish(levels, parts, surplus, got_near, got_far)),
    )
    return updated, coefficients.reshape(-1)


def solution(mesh):
    torus = Mesh(
        mesh.devices.reshape(mesh.shape["grp"], 8, 8, 2, 2),
        ("grp", *DOM),
    )
    return jax.shard_map(
        whole,
        mesh=torus,
        in_specs=(P("grp", None, DOM), P("grp", None)),
        out_specs=(P("grp", None, DOM), P()),
        check_vma=False,
    )
```
